32 devices in a mesh: site: 2 (over y), pts: 16 (over z, x, core).
Axes of the slice: x: 2, y: 2, z: 4, core: 2. Of those that a mesh axis runs over, the one named last changes fastest.
Arguments:
- green_tensors: bfloat16 [512, 4, 6, 2, 1024], P(('site', 'pts')), parts along dimension 0, may hold values from -6 to 6
- block_lists: int32 [32, 32], P(('site', 'pts')), parts along dimension 0, may hold values from 0 to 255, as said below
- block_count: int32 [32], P(('site', 'pts')), parts along dimension 0, may hold values from 1 to 32
- onset_steps: int32 [32, 16, 128], P(('site', 'pts')), parts along dimension 0, may hold values from 0 to 255
- slip_amount: float32 [32, 16, 128], P(('site', 'pts')), parts along dimension 0, may hold values from 0.2 to 2
- mechanism: float32 [32, 6], P(('site', 'pts')), parts along dimension 0, may hold values from -2.4 to 2.4
- slip_rate: float32 [32, 16, 128], P(('site', 'pts')), parts along dimension 0, may hold values from 0.005 to 0.05
Outputs:
- seismograms: float32 [32, 16, 2, 1024], P(('site', 'pts')), parts along dimension 0
The draws below stay inside these ranges and needn't reach their ends.
There are 2 independent parts, one for each index of `site`. The reference program is written for one: setup_inputs(seed, part) draws one part's arguments, and reference() takes and returns one part's arrays. A program takes and returns all parts, laid end to end along the dimension named above; each array names one. Nothing has to cross between parts.
Inputs may be any that keep to these rules, and one draw needn't show every extreme that they name: `block_lists`: numbers of point blocks; the ruptures held by one device name at most 2 entries in blocks held by any one device, and exactly 2 for some holder.
All inputs are finite; a program needn't handle non-finite values.
Results may differ from the reference program's by a relative error of at most 0.0003.
Values may be sent and summed in bfloat16 or wider, within the bound.
A program may use at most 128 MiB of HBM per device.

```python
import math
import jax
import jax.numpy as jnp
from jax import lax

NT = 1024
P_SIZE = 4
K = 32
V = 16
L = 128
MAXON = 256
BD = 16
RD = 1
NB = 256
R = 16
N_PTS = 16


def draw_block_lists(key, part):
    entries = RD * K

    def per_worker(worker):
        worker_key = jax.random.fold_in(jax.random.fold_in(key, 11), worker)
        holders = jax.random.permutation(worker_key, N_PTS)
        order = jnp.arange(entries, dtype=jnp.int32)
        holder_of = holders[order % N_PTS]
        local_block = jax.random.randint(jax.random.fold_in(worker_key, 1), (entries,), 0, BD)
        return (holder_of * BD + local_block).astype(jnp.int32)
    lists = jax.vmap(per_worker)(jnp.arange(N_PTS, dtype=jnp.int32))
    return lists.reshape(RD * N_PTS, K)


def set_ends(values, own_key, low, top_value):
    index_at = [jax.random.randint(jax.random.fold_in(own_key, axis), (), 0, length) for axis, length in enumerate(values.shape)]
    main_axis = values.shape.index(max(values.shape))
    beside = index_at[:main_axis] + [(index_at[main_axis] + 1) % values.shape[main_axis]] + index_at[main_axis + 1:]
    return values.at[tuple(index_at)].set(low).at[tuple(beside)].set(top_value)


def steps_of(own_key, dims, cuts, smallest, top_value):
    def one(dim, blocks):
        draws = jax.random.uniform(jax.random.fold_in(jax.random.fold_in(own_key, 6), dim), (blocks,), jnp.float32, smallest / len(cuts), top_value / len(cuts))
        return jnp.repeat(jnp.exp(draws), dims[dim] // blocks).reshape((-1,) + (1,) * (len(dims) - dim - 1))

    gain = one(*cuts[0])
    for cut in cuts[1:]:
        gain = gain * one(*cut)
    return gain


def normal_values(rng, shape, scale, limit, cuts=(), kind=jnp.bfloat16):
    array = scale * jax.random.normal(rng, shape, jnp.float32)
    if cuts:
        array = array * steps_of(rng, shape, cuts, -0.22, 0.18)
    return jnp.clip(array, -limit, limit).astype(kind)


def setup_inputs(seed: int = 0, part: int = 0) -> dict:
    keys = jax.random.split(jax.random.key(seed), 8)
    part_keys = jax.random.split(jax.random.fold_in(keys[7], part), 8)
    return {
        "green_tensors": normal_values(part_keys[0], (NB, P_SIZE, 6, 2, NT), 1.0, 6.0, ((0, 16),)),
        "block_lists": draw_block_lists(jax.random.fold_in(jax.random.fold_in(keys[7], part), 71), part),
        "block_count": set_ends(jax.random.randint(part_keys[2], (R,), 1, K + 1), jax.random.fold_in(part_keys[2], 1), 1, K).astype(jnp.int32),
        "onset_steps": set_ends(jax.random.randint(part_keys[3], (R, V, K * P_SIZE), 0, MAXON), jax.random.fold_in(part_keys[3], 1), 0, MAXON - 1).astype(jnp.int32),
        "slip_amount": jnp.clip(jnp.exp(math.log(2.0) - 2.3025851 * jax.random.uniform(part_keys[4], (R, V, K * P_SIZE), jnp.float32) ** steps_of(part_keys[4], (R, V, K * P_SIZE), ((0, 16),), -0.2, 0.2)), 0.2, 2.0),
        "mechanism": normal_values(part_keys[5], (R, 6), 0.4, 2.4, ((0, 16),), jnp.float32),
        "slip_rate": jnp.clip(jnp.exp(math.log(0.05) - 2.3025851 * jax.random.uniform(part_keys[6], (R, V, L), jnp.float32) ** steps_of(part_keys[6], (R, V, L), ((0, 16),), -0.2, 0.2)), 0.005, 0.05),
    }


def lag_traces(traces, onsets):
    steps = jnp.arange(traces.shape[-1], dtype=jnp.int32)
    source = steps[None, :] - onsets[:, None]
    inside = source >= 0
    picked = jnp.take_along_axis(traces, jnp.broadcast_to(jnp.maximum(source, 0)[:, None, :], traces.shape), axis=2)
    return jnp.where(inside[:, None, :], picked, 0.0)


def weighted_sum(traces, weights, onsets):
    def per_variation(weight_row, onset_row):
        return jnp.sum(weight_row[:, None, None] * lag_traces(traces, onset_row), axis=0)
    return jax.vmap(per_variation)(weights, onsets)


def reference(green_tensors, block_lists, block_count, onset_steps, slip_amount, mechanism, slip_rate):
    listed = block_lists.shape[1]
    length = green_tensors.shape[-1]

    def per_rupture(inputs):
        blocks, listed_count, onset_rows, slip_rows, mech_row, rate_rows = inputs
        chosen = jnp.take(green_tensors, blocks, axis=0).astype(jnp.float32)
        traces = jnp.einsum("kpsct,s->kpct", chosen, mech_row, precision=lax.Precision.HIGHEST)
        kept_mask = (jnp.arange(listed, dtype=jnp.int32) < listed_count).astype(jnp.float32)
        points = chosen.shape[1]
        weights = slip_rows * jnp.repeat(kept_mask, points)[None, :]
        motion = weighted_sum(traces.reshape(-1, 2, length), weights, onset_rows)

        def convolve_row(signal, kernel):
            return jnp.convolve(signal, kernel, precision=lax.Precision.HIGHEST)[:length]

        return jax.vmap(jax.vmap(convolve_row, (0, None)), (0, 0))(motion, rate_rows)

    return lax.map(per_rupture, (block_lists, block_count, onset_steps, slip_amount, mechanism, slip_rate))
```

```python
import functools

import jax
import jax.numpy as jnp
from jax import lax
from jax.experimental import pallas as pl
from jax.experimental.pallas import tpu as pltpu
from jax.sharding import PartitionSpec as P

LANES = 128
TOP = 32766.0


def seismogram_kernel(n, plane, cap, held, points, comps,
                      count_s, list_hbm, mech_hbm, green_hbm, onset_hbm, slip_hbm, rate_hbm, out_ref,
                      list_v, mech_v, mech_row, green, onset_v, slip_v, rate_v,
                      table, own_v, own_s, want_v, gain_v, outbox, out_scale, inbox, in_scale,
                      motion, high_taps, low_taps, source_of, back_of, weight_of, meta_bytes, trace_bytes,
                      local_sem, far_sem, send_m, recv_m, send_t, recv_t):
    me = lax.axis_index("pts")
    planes = n // plane
    z = me // plane
    i_own = me % plane
    toward = jnp.where(z < planes // 2, 1, -1)
    listed = list_hbm.shape[-1]
    strains = mech_hbm.shape[-1]
    variations, rows = out_ref.shape[0], out_ref.shape[1]
    tiles = rows // comps
    half = rows // 2
    mesh_id = pl.DeviceIdType.MESH

    barrier = pltpu.get_barrier_semaphore()

    def inside(q):
        return jnp.logical_and(q >= 0, q < planes)

    def in_plane(q, action):
        def body(t, carry):
            action(q * plane + (i_own + t) % plane)
            return carry

        @pl.when(inside(q))
        def _():
            lax.fori_loop(0, plane, body, 0, unroll=True)

    def beside(action):
        def body(t, carry):
            action(z * plane + (i_own + t) % plane)
            return carry

        lax.fori_loop(1, plane, body, 0, unroll=True)

    def greet(there):
        pl.semaphore_signal(barrier, inc=1, device_id={"pts": there}, device_id_type=mesh_id)

    in_plane(z + toward, greet)
    in_plane(z - toward, greet)
    beside(greet)

    local_copies = [
        pltpu.make_async_copy(src, dst, local_sem.at[i]) for i, (src, dst) in enumerate([
            (list_hbm, list_v), (mech_hbm, mech_v),
            (onset_hbm, onset_v), (slip_hbm, slip_v), (rate_hbm, rate_v), (green_hbm, green)])]
    for copy in local_copies:
        copy.start()
    for copy in local_copies[:2]:
        copy.wait()

    slots = n * cap

    def holder_of(blocks):
        if held & (held - 1) == 0:
            return jnp.right_shift(blocks, held.bit_length() - 1)
        return sum((blocks >= h * held).astype(jnp.int32) for h in range(1, n))

    k_across = lax.broadcasted_iota(jnp.int32, (listed, listed), 1)
    k_down = lax.broadcasted_iota(jnp.int32, (listed, listed), 0)
    as_row = jnp.broadcast_to(list_v[...], (listed, listed))
    as_col = jnp.sum(jnp.where(k_across == k_down, as_row, 0), axis=1, keepdims=True)
    holder_row = holder_of(as_row)
    holder_col = holder_of(as_col)
    same = holder_row == holder_col
    rank_row = jnp.sum(jnp.where(jnp.logical_and(same, k_down < k_across), 1, 0), axis=0, keepdims=True)
    rank_col = jnp.sum(jnp.where(jnp.logical_and(same, k_across < k_down), 1, 0), axis=1, keepdims=True)
    slot_down = lax.broadcasted_iota(jnp.int32, (slots, listed), 0)
    slot_row = holder_row[0:1] * cap + rank_row
    block_row = as_row[0:1] - holder_row[0:1] * held
    hit = slot_down == jnp.broadcast_to(slot_row, (slots, listed))
    block_col = jnp.sum(jnp.where(hit, jnp.broadcast_to(block_row, (slots, listed)), 0), axis=1, keepdims=True)
    block_col = jnp.broadcast_to(block_col, (slots, LANES))
    for h in range(n):
        table[h] = block_col[h * cap:(h + 1) * cap]
    mech_row[...] = jnp.zeros(mech_row.shape, jnp.float32)
    mech_row[:, 0:strains] = mech_v[...]

    has_low = jnp.where(z > 0, 1, 0)
    has_high = jnp.where(z < planes - 1, 1, 0)
    pl.semaphore_wait(barrier, plane - 1 + plane * (has_low + has_high))

    def remote(src, dst, send, recv, there):
        return pltpu.make_async_remote_copy(
            src_ref=src, dst_ref=dst, send_sem=send, recv_sem=recv,
            device_id={"pts": there}, device_id_type=mesh_id)

    def tell(k):
        for sign in (-1, 1):
            q = z + sign * k

            @pl.when(jnp.logical_and(inside(q), inside(z - sign)))
            def _():
                pl.semaphore_signal(far_sem.at[q], inc=1, device_id={"pts": me - sign * plane},
                                    device_id_type=mesh_id)

    def start_meta(there):
        remote(table.at[there], want_v.at[me], send_m, recv_m.at[z], there).start()
        remote(mech_row, gain_v.at[me], send_m, recv_m.at[z], there).start()

    def wait_meta(q):
        pltpu.make_async_copy(meta_bytes, meta_bytes, recv_m.at[q]).wait()

    def make_taps():
        i_row = lax.broadcasted_iota(jnp.int32, (LANES, LANES), 0)
        j_lane = lax.broadcasted_iota(jnp.int32, (LANES, LANES), 1)
        near_mask = j_lane >= i_row
        motion[...] = jnp.zeros(motion.shape, jnp.float32)

        def taps(v, carry):
            rate = jnp.broadcast_to(rate_v[pl.ds(v, 1), :], (LANES, LANES))
            turned = pltpu.roll(rate, 0, 1, stride=1, stride_axis=0)
            both = jnp.concatenate(
                [jnp.where(near_mask, turned, 0.0), jnp.where(near_mask, 0.0, turned)], axis=0)
            high = both.astype(jnp.bfloat16)
            high_taps[v] = high
            low_taps[v] = (both - high.astype(jnp.float32)).astype(jnp.bfloat16)
            return carry

        lax.fori_loop(0, variations, taps, 0, unroll=4)

    def spread_points():
        lane = lax.broadcasted_iota(jnp.int32, (variations, LANES), 1)
        count = count_s[0]
        onsets = onset_v[...]
        slips = slip_v[...]

        def spread(q, carry):
            pick = jnp.full((variations, LANES), q, jnp.int32)
            onset = jnp.take_along_axis(onsets, pick, axis=1)
            slip = jnp.take_along_axis(slips, pick, axis=1)
            shift = jnp.bitwise_and(onset, LANES - 1)
            source_of[q] = lane - shift
            back_of[q] = jnp.right_shift(onset, 7) + (lane >= LANES - shift).astype(jnp.int32)
            used = jnp.where(pick < count * points, 1.0, 0.0)
            weight_of[q] = slip * used
            return carry

        lax.fori_loop(0, listed * points, spread, 0, unroll=16)
        for p in range(points):
            source_of[listed * points + p] = lane
            back_of[listed * points + p] = jnp.zeros((variations, LANES), jnp.int32)
            weight_of[listed * points + p] = jnp.zeros((variations, LANES), jnp.float32)

    tell(1)
    in_plane(z + toward, start_meta)
    in_plane(z - toward, start_meta)

    def reach(k, carry):
        for sign in (-1, 1):
            q = z + sign * k

            @pl.when(inside(q))
            def _():
                pl.semaphore_wait(far_sem.at[q], 1)

        tell(k)
        in_plane(z + toward * k, start_meta)
        in_plane(z - toward * k, start_meta)
        return carry

    beside(start_meta)
    for copy in local_copies[4:5]:
        copy.wait()
    make_taps()
    if planes > 2:
        reach(2, 0)
    for copy in local_copies[2:4]:
        copy.wait()
    spread_points()
    lax.fori_loop(3, planes, reach, 0)

    as_k = lax.broadcasted_iota(jnp.int32, (listed, LANES), 0)
    lane_slot = lax.broadcasted_iota(jnp.int32, (listed, LANES), 1)
    mine = lane_slot == holder_col * cap + rank_col
    own_v[...] = jnp.sum(jnp.where(mine, as_k - listed, 0), axis=0, keepdims=True) + listed
    to_scalar = pltpu.make_async_copy(own_v, own_s, local_sem.at[6])
    to_scalar.start()
    local_copies[5].wait()

    def encode(wants, gains, box, scale_box, at):
        gain = gains
        gain = [jnp.broadcast_to(gain[:, s:s + 1], (rows, LANES)) for s in range(strains)]
        for slot in range(cap):
            block = wants[slot, 0]
            traces = []
            for p in range(points):
                total = gain[0] * green[block, p, 0].astype(jnp.float32)
                for s in range(1, strains):
                    total += gain[s] * green[block, p, s].astype(jnp.float32)
                traces.append(total)
            top = jnp.abs(traces[0])
            for part in traces[1:]:
                top = jnp.maximum(top, jnp.abs(part))
            top = jnp.max(jnp.max(top, axis=0, keepdims=True), axis=1, keepdims=True)
            top = jnp.broadcast_to(jnp.maximum(top, 1e-30), (1, LANES))
            scale_box[at, :, slot * LANES:(slot + 1) * LANES] = top * (1.0 / (TOP * 65536.0))
            inverse = jnp.broadcast_to(TOP / top, (half, LANES))
            for p in range(points):
                low = lax.round(traces[p][:half] * inverse, lax.RoundingMethod.TO_NEAREST_EVEN)
                high = lax.round(traces[p][half:] * inverse - low * (1.0 / 65536.0),
                                 lax.RoundingMethod.TO_NEAREST_EVEN)
                box[at, slot, p] = jnp.left_shift(high.astype(jnp.int32), 16) + low.astype(jnp.int32)

    def encode_to(there):
        encode(want_v[there], gain_v[there], outbox, out_scale, there)
        remote(outbox.at[there], inbox.at[me], send_t, recv_t.at[me], there).start()
        remote(out_scale.at[there], in_scale.at[me], send_t, recv_t.at[me], there).start()

    def encode_far(t, carry):
        ring = t // plane
        q = z + jnp.where(ring % 2 == 0, toward, -toward) * (ring // 2 + 1)

        @pl.when(inside(q))
        def _():
            @pl.when(t % plane == 0)
            def _():
                wait_meta(q)

            encode_to(q * plane + (i_own + t) % plane)

        return carry

    lax.fori_loop(0, 2 * (planes - 1) * plane, encode_far, 0)

    if plane > 1:
        beside_bytes = meta_bytes.at[pl.ds(0, (plane - 1) * (cap + 1))]
        pltpu.make_async_copy(beside_bytes, beside_bytes, recv_m.at[z]).wait()

    def encode_plane(t, carry):
        encode_to(z * plane + (i_own + t) % plane)
        return carry

    lax.fori_loop(1, plane, encode_plane, 0)
    encode(table[me], mech_row[...], inbox, in_scale, me)
    to_scalar.wait()

    depth = tiles // 2

    def add_traces(js):
        bases = [own_s[0, j * cap + slot] * points for j in js for slot in range(cap)]
        scales = [jnp.broadcast_to(in_scale[j, :, slot * LANES:(slot + 1) * LANES], (8, LANES))
                  for j in js for slot in range(cap)]
        for group in range(variations // 8):
            part = slice(group * 8, group * 8 + 8)
            acc = [motion[comps + q, part, :] for q in range(rows)]
            for e, (base, scale) in enumerate(zip(bases, scales)):
                j, slot = js[e // cap], e % cap
                for p in range(points):
                    source = jnp.bitwise_and(source_of[base + p, part, :], LANES - 1)
                    back = back_of[base + p, part, :]
                    weight = weight_of[base + p, part, :] * scale
                    one = back >= 1
                    two = back >= 2
                    for c in range(comps):
                        words = [jnp.broadcast_to(
                            inbox[j, slot, p, i * comps + c:i * comps + c + 1, :], (8, LANES))
                            for i in range(depth)]
                        prev2 = jnp.left_shift(words[depth - 2], 16)
                        prev1 = jnp.left_shift(words[depth - 1], 16)
                        for i in range(depth):
                            cur = words[i]
                            mixed = jnp.where(two, prev2, jnp.where(one, prev1, cur))
                            moved = jnp.take_along_axis(mixed, source, axis=1)
                            row = i * comps + c
                            acc[row] += weight * jnp.left_shift(moved, 16).astype(jnp.float32)
                            acc[row + half] += weight * moved.astype(jnp.float32)
                            prev2, prev1 = prev1, cur
            for q in range(rows):
                motion[comps + q, part, :] = acc[q]

    pair = 2 if plane % 2 == 0 else 1

    def arrive(t, carry):
        ring = t // (plane // pair)
        k = (ring + 1) // 2
        q = z + jnp.where(ring % 2 == 1, -toward, toward) * k
        first = q * plane + ((i_own // pair + t) % (plane // pair)) * pair

        @pl.when(inside(q))
        def _():
            for j in [first + d for d in range(pair)]:
                @pl.when(j != me)
                def _():
                    pltpu.make_async_copy(trace_bytes, trace_bytes, recv_t.at[j]).wait()

            add_traces([first + d for d in range(pair)])

        return carry

    lax.fori_loop(0, (2 * planes - 1) * (plane // pair), arrive, 0)

    for v in range(variations):
        lhs = jnp.concatenate([motion[comps:comps + rows, v, :], motion[0:rows, v, :]], axis=1)
        high = lhs.astype(jnp.bfloat16).astype(jnp.float32)
        pair = jnp.concatenate([high, lhs - high], axis=0).astype(jnp.bfloat16)
        main = jnp.dot(pair, high_taps[v], preferred_element_type=jnp.float32)
        minor = jnp.dot(pair[:rows], low_taps[v], preferred_element_type=jnp.float32)
        out_ref[v] = main[:rows] + (main[rows:] + minor)

    others = pl.ds(0, n - 1)
    for box, sem in ((want_v, send_m), (gain_v, send_m), (outbox, send_t), (out_scale, send_t)):
        pltpu.make_async_copy(box.at[others], box.at[others], sem).wait()


def local(plane, green_tensors, block_lists, block_count, onset_steps, slip_amount, mechanism, slip_rate):
    held, points, strains, comps, length = green_tensors.shape
    ruptures, listed = block_lists.shape
    assert ruptures == 1
    variations = onset_steps.shape[1]
    n = lax.axis_size("pts")
    cap = max(1, listed // n)
    tiles = length // LANES
    rows = tiles * comps
    assert n * cap <= LANES and listed * points <= LANES and rows == 16 and variations % 8 == 0
    green = green_tensors.reshape(held, points, strains, comps, tiles, LANES)
    green = green.transpose(0, 1, 2, 4, 3, 5).reshape(held, points, strains, rows, LANES)

    hbm = pl.BlockSpec(memory_space=pltpu.MemorySpace.HBM)
    vmem = pl.BlockSpec(memory_space=pltpu.VMEM)
    dma = pltpu.SemaphoreType.DMA
    planes = n // plane
    seismograms = pl.pallas_call(
        functools.partial(seismogram_kernel, n, plane, cap, held, points, comps),
        out_shape=jax.ShapeDtypeStruct((variations, rows, LANES), jnp.float32),
        in_specs=[pl.BlockSpec(memory_space=pltpu.SMEM)] + [hbm] * 6,
        out_specs=vmem,
        scratch_shapes=[
            pltpu.VMEM((1, listed), jnp.int32),
            pltpu.VMEM((1, strains), jnp.float32),
            pltpu.VMEM((1, LANES), jnp.float32),
            pltpu.VMEM((held, points, strains, rows, LANES), jnp.bfloat16),
            pltpu.VMEM((variations, listed * points), jnp.int32),
            pltpu.VMEM((variations, listed * points), jnp.float32),
            pltpu.VMEM((variations, LANES), jnp.float32),
            pltpu.VMEM((n, cap, LANES), jnp.int32),
            pltpu.VMEM((1, LANES), jnp.int32),
            pltpu.SMEM((1, LANES), jnp.int32),
            pltpu.VMEM((n, cap, LANES), jnp.int32),
            pltpu.VMEM((n, 1, LANES), jnp.float32),
            pltpu.VMEM((n, cap, points, rows // 2, LANES), jnp.int32),
            pltpu.VMEM((n, 1, cap * LANES), jnp.float32),
            pltpu.VMEM((n, cap, points, rows // 2, LANES), jnp.int32),
            pltpu.VMEM((n, 1, cap * LANES), jnp.float32),
            pltpu.VMEM((rows + comps, variations, LANES), jnp.float32),
            pltpu.VMEM((variations, 2 * LANES, LANES), jnp.bfloat16),
            pltpu.VMEM((variations, 2 * LANES, LANES), jnp.bfloat16),
            pltpu.VMEM(((listed + 1) * points, variations, LANES), jnp.int32),
            pltpu.VMEM(((listed + 1) * points, variations, LANES), jnp.int32),
            pltpu.VMEM(((listed + 1) * points, variations, LANES), jnp.float32),
            pltpu.VMEM((plane * (cap + 1), 1, LANES), jnp.int32),
            pltpu.VMEM((cap * (points * rows // 2 + 1), 1, LANES), jnp.int32),
            dma((7,)), pltpu.SemaphoreType.REGULAR((planes,)), dma, dma((planes,)), dma, dma((n,)),
        ],
        compiler_params=pltpu.CompilerParams(
            collective_id=0, has_side_effects=True, vmem_limit_bytes=32 << 20),
        name="seismograms",
    )(block_count, *(pltpu.with_memory_space_constraint(x, pltpu.MemorySpace.HBM) for x in (
        block_lists, mechanism, green, onset_steps[0], slip_amount[0], slip_rate[0])))
    out = seismograms.reshape(variations, tiles, comps, LANES).transpose(0, 2, 1, 3)
    return out.reshape(1, variations, comps, length)


def solution(mesh):
    n = mesh.shape["pts"]
    line = mesh.devices.reshape(-1, n)[0]
    heights = [getattr(d, "coords", (0, 0, 0))[2] for d in line]
    plane = sum(1 for h in heights if h == heights[0])
    assert n % plane == 0
    in_specs = (
        P(("site", "pts"), None, None, None, None),
        P(("site", "pts"), None),
        P(("site", "pts")),
        P(("site", "pts"), None, None),
        P(("site", "pts"), None, None),
        P(("site", "pts"), None),
        P(("site", "pts"), None, None),
    )
    out_specs = P(("site", "pts"), None, None, None)
    return jax.shard_map(functools.partial(local, plane), mesh=mesh, in_specs=in_specs, out_specs=out_specs,
                         check_vma=False)
```

```python
import functools

import jax
import jax.numpy as jnp
from jax import lax
from jax.experimental import pallas as pl
from jax.experimental.pallas import tpu as pltpu
from jax.sharding import PartitionSpec as P

LANES = 128
TOP = 32766.0
SLIP = 32767.0


def seismogram_kernel(n, plane, cap, held, points, comps,
                      count_s, list_hbm, mech_hbm, green_hbm, onset_hbm, slip_hbm, rate_hbm, out_ref,
                      list_v, mech_v, mech_row, green, onset_v, slip_v, rate_v,
                      table, want_v, gain_v, word_out, word_in, box, scale_box, sum_out, sum_in, top_out, top_in,
                      total, motion, high_taps, low_taps, source_of, back_of, weight_of, meta_bytes, trace_bytes,
                      sum_bytes, local_sem, far_sem, send_m, recv_m, send_w, recv_w, send_t, recv_t, send_p, recv_p):
    me = lax.axis_index("pts")
    planes = n // plane
    z = me // plane
    i_own = me % plane
    toward = jnp.where(z < planes // 2, 1, -1)
    listed = list_hbm.shape[-1]
    strains = mech_hbm.shape[-1]
    variations, rows = out_ref.shape[0], out_ref.shape[1]
    tiles = rows // comps
    half = rows // 2
    depth = tiles // 2
    width = plane * cap * points
    fold = LANES // width
    folded = variations // fold
    mesh_id = pl.DeviceIdType.MESH
    nearest = lax.RoundingMethod.TO_NEAREST_EVEN

    barrier = pltpu.get_barrier_semaphore()

    def inside(q):
        return jnp.logical_and(q >= 0, q < planes)

    def in_plane(q, action):
        def body(t, carry):
            action(q * plane + (i_own + t) % plane)
            return carry

        @pl.when(inside(q))
        def _():
            lax.fori_loop(0, plane, body, 0, unroll=True)

    def beside(action):
        def body(t, carry):
            action(z * plane + (i_own + t) % plane)
            return carry

        lax.fori_loop(1, plane, body, 0, unroll=True)

    def greet(there):
        pl.semaphore_signal(barrier, inc=1, device_id={"pts": there}, device_id_type=mesh_id)

    in_plane(z + toward, greet)
    in_plane(z - toward, greet)
    beside(greet)

    local_copies = [
        pltpu.make_async_copy(src, dst, local_sem.at[i]) for i, (src, dst) in enumerate([
            (list_hbm, list_v), (mech_hbm, mech_v),
            (onset_hbm, onset_v), (slip_hbm, slip_v), (rate_hbm, rate_v), (green_hbm, green)])]
    for copy in local_copies:
        copy.start()
    for copy in local_copies[:2]:
        copy.wait()

    slots = n * cap

    def holder_of(blocks):
        if held & (held - 1) == 0:
            return jnp.right_shift(blocks, held.bit_length() - 1)
        return sum((blocks >= h * held).astype(jnp.int32) for h in range(1, n))

    k_across = lax.broadcasted_iota(jnp.int32, (listed, listed), 1)
    k_down = lax.broadcasted_iota(jnp.int32, (listed, listed), 0)
    as_row = jnp.broadcast_to(list_v[...], (listed, listed))
    as_col = jnp.sum(jnp.where(k_across == k_down, as_row, 0), axis=1, keepdims=True)
    holder_row = holder_of(as_row)
    holder_col = holder_of(as_col)
    same = holder_row == holder_col
    rank_row = jnp.sum(jnp.where(jnp.logical_and(same, k_down < k_across), 1, 0), axis=0, keepdims=True)
    rank_col = jnp.sum(jnp.where(jnp.logical_and(same, k_across < k_down), 1, 0), axis=1, keepdims=True)
    slot_down = lax.broadcasted_iota(jnp.int32, (slots, listed), 0)
    slot_row = holder_row[0:1] * cap + rank_row
    block_row = as_row[0:1] - holder_row[0:1] * held
    hit = slot_down == jnp.broadcast_to(slot_row, (slots, listed))
    block_col = jnp.sum(jnp.where(hit, jnp.broadcast_to(block_row, (slots, listed)), 0), axis=1, keepdims=True)
    block_col = jnp.broadcast_to(block_col, (slots, LANES))
    for h in range(n):
        table[h] = block_col[h * cap:(h + 1) * cap]
    mech_row[...] = jnp.zeros(mech_row.shape, jnp.float32)
    mech_row[:, 0:strains] = mech_v[...]

    has_low = jnp.where(z > 0, 1, 0)
    has_high = jnp.where(z < planes - 1, 1, 0)
    pl.semaphore_wait(barrier, plane - 1 + plane * (has_low + has_high))

    def remote(src, dst, send, recv, there):
        return pltpu.make_async_remote_copy(
            src_ref=src, dst_ref=dst, send_sem=send, recv_sem=recv,
            device_id={"pts": there}, device_id_type=mesh_id)

    def await_bytes(ref, sem):
        pltpu.make_async_copy(ref, ref, sem).wait()

    def tell(k):
        for sign in (-1, 1):
            q = z + sign * k

            @pl.when(jnp.logical_and(inside(q), inside(z - sign)))
            def _():
                pl.semaphore_signal(far_sem.at[q], inc=1, device_id={"pts": me - sign * plane},
                                    device_id_type=mesh_id)

    def start_meta(there):
        remote(table.at[there], want_v.at[me], send_m, recv_m.at[z], there).start()
        remote(mech_row, gain_v.at[me], send_m, recv_m.at[z], there).start()

    def start_words(q):
        @pl.when(inside(q))
        def _():
            remote(word_out.at[q], word_in.at[z], send_w, recv_w.at[z], q * plane + i_own).start()

    tell(1)
    in_plane(z + toward, start_meta)
    in_plane(z - toward, start_meta)
    beside(start_meta)
    want_v[me] = table[me]
    gain_v[me] = mech_row[...]

    def make_words():
        lane = lax.broadcasted_iota(jnp.int32, (1, LANES), 1)
        as_k = lax.broadcasted_iota(jnp.int32, (listed, LANES), 0)
        entry = jnp.bitwise_and(lane, width - 1)
        in_slot = jnp.right_shift(entry, points.bit_length() - 1)
        slot_col = jnp.broadcast_to(holder_col * cap + rank_col, (listed, LANES))
        slip = lax.round(slip_v[...] * SLIP, nearest).astype(jnp.int32)
        packed = jnp.bitwise_or(jnp.left_shift(onset_v[...], 16), slip)
        count = count_s[0]
        for q in range(planes):
            mine = slot_col == jnp.broadcast_to(in_slot + q * plane * cap, (listed, LANES))
            k = jnp.sum(jnp.where(mine, as_k - listed, 0), axis=0, keepdims=True) + listed
            pick = jnp.minimum(k, listed - 1) * points + jnp.bitwise_and(entry, points - 1)
            words = jnp.take_along_axis(packed, jnp.broadcast_to(pick, (variations, LANES)), axis=1)
            words = jnp.where(jnp.broadcast_to(k < count, (variations, LANES)), words, 0)
            kept = words[0:folded]
            for b in range(1, fold):
                there = jnp.broadcast_to(lane >= b * width, (folded, LANES))
                kept = jnp.where(there, words[b * folded:(b + 1) * folded], kept)
            word_out[q] = kept
        word_in[z] = word_out[z]

    def make_taps():
        i_row = lax.broadcasted_iota(jnp.int32, (LANES, LANES), 0)
        j_lane = lax.broadcasted_iota(jnp.int32, (LANES, LANES), 1)
        near_mask = j_lane >= i_row

        def taps(v, carry):
            rate = jnp.broadcast_to(rate_v[pl.ds(v, 1), :], (LANES, LANES))
            turned = pltpu.roll(rate, 0, 1, stride=1, stride_axis=0)
            both = jnp.concatenate(
                [jnp.where(near_mask, turned, 0.0), jnp.where(near_mask, 0.0, turned)], axis=0)
            high = both.astype(jnp.bfloat16)
            high_taps[v] = high
            low_taps[v] = (both - high.astype(jnp.float32)).astype(jnp.bfloat16)
            return carry

        lax.fori_loop(0, variations, taps, 0, unroll=4)

    def reach(k, carry):
        for sign in (-1, 1):
            q = z + sign * k

            @pl.when(inside(q))
            def _():
                pl.semaphore_wait(far_sem.at[q], 1)

        tell(k)
        in_plane(z + toward * k, start_meta)
        in_plane(z - toward * k, start_meta)
        start_words(z + toward * k)
        start_words(z - toward * k)
        return carry

    for copy in local_copies[2:4]:
        copy.wait()
    make_words()
    start_words(z + toward)
    start_words(z - toward)
    if planes > 2:
        reach(2, 0)
    local_copies[4].wait()
    make_taps()
    motion[0:comps] = jnp.zeros((comps, variations, LANES), jnp.float32)
    lax.fori_loop(3, planes, reach, 0)
    local_copies[5].wait()

    def encode(r, at):
        gain = gain_v[r]
        gain = [jnp.broadcast_to(gain[:, s:s + 1], (rows, LANES)) for s in range(strains)]
        wants = want_v[r]
        for slot in range(cap):
            block = wants[slot, 0]
            traces = []
            for p in range(points):
                trace = gain[0] * green[block, p, 0].astype(jnp.float32)
                for s in range(1, strains):
                    trace += gain[s] * green[block, p, s].astype(jnp.float32)
                traces.append(trace)
            top = jnp.abs(traces[0])
            for part in traces[1:]:
                top = jnp.maximum(top, jnp.abs(part))
            top = jnp.max(jnp.max(top, axis=0, keepdims=True), axis=1, keepdims=True)
            top = jnp.broadcast_to(jnp.maximum(top, 1e-30), (1, LANES))
            scale_box[at, :, slot * LANES:(slot + 1) * LANES] = top * (1.0 / (TOP * 65536.0))
            inverse = jnp.broadcast_to(TOP / top, (half, LANES))
            for p in range(points):
                low = lax.round(traces[p][:half] * inverse, nearest)
                high = lax.round(traces[p][half:] * inverse - low * (1.0 / 65536.0), nearest)
                box[at, slot, p] = jnp.left_shift(high.astype(jnp.int32), 16) + low.astype(jnp.int32)

    last_ring = 2 * (planes - 1)

    def plane_of(ring):
        k = jnp.where(ring == last_ring, 0, ring // 2 + 1)
        return z + jnp.where(ring % 2 == 0, toward, -toward) * k

    def encode_all(t, carry):
        ring = t // plane
        q = plane_of(ring)

        @pl.when(inside(q))
        def _():
            @pl.when(jnp.logical_and(t % plane == 0, q != z))
            def _():
                await_bytes(meta_bytes, recv_m.at[q])

            if plane > 1:
                @pl.when(jnp.logical_and(t % plane == 0, q == z))
                def _():
                    await_bytes(meta_bytes.at[pl.ds(0, (plane - 1) * (cap + 1))], recv_m.at[q])

            i = (i_own + t + 1) % plane
            r = q * plane + i
            encode(r, jnp.where(i == i_own, r + n, r))

            @pl.when(i != i_own)
            def _():
                there = z * plane + i
                slot = q * plane + i_own
                remote(box.at[r], box.at[n + slot], send_t, recv_t.at[slot], there).start()
                remote(scale_box.at[r], scale_box.at[n + slot], send_t, recv_t.at[slot], there).start()

        return carry

    lax.fori_loop(0, (2 * planes - 1) * plane, encode_all, 0)

    def spread(q):
        words = word_in[q]
        words = jnp.concatenate([words] * fold, axis=0)
        lane = lax.broadcasted_iota(jnp.int32, (variations, LANES), 1)
        start = lax.broadcasted_iota(jnp.int32, (variations, LANES), 0) // folded * width
        for e in range(width):
            word = jnp.take_along_axis(words, start + e, axis=1)
            onset = jnp.right_shift(word, 16)
            shift = jnp.bitwise_and(onset, LANES - 1)
            source_of[e] = lane - shift
            back_of[e] = jnp.right_shift(onset, 7) + (lane >= LANES - shift).astype(jnp.int32)
            weight_of[e] = jnp.bitwise_and(word, 0xFFFF).astype(jnp.float32) * (1.0 / SLIP)

    pair = 2 if plane % 2 == 0 else 1

    def add_traces(q, i_first):
        for group in range(variations // 8):
            part = slice(group * 8, group * 8 + 8)
            acc = [total[r, part, :] for r in range(rows)]
            for e in range(pair * cap):
                at = n + q * plane + i_first + e // cap
                slot = e % cap
                scale = jnp.broadcast_to(scale_box[at, :, slot * LANES:(slot + 1) * LANES], (8, LANES))
                for p in range(points):
                    entry = (i_first * cap + e) * points + p
                    source = jnp.bitwise_and(source_of[entry, part, :], LANES - 1)
                    back = back_of[entry, part, :]
                    weight = weight_of[entry, part, :] * scale
                    one = back >= 1
                    two = back >= 2
                    for c in range(comps):
                        words = [jnp.broadcast_to(
                            box[at, slot, p, i * comps + c:i * comps + c + 1, :], (8, LANES))
                            for i in range(depth)]
                        prev2 = jnp.left_shift(words[depth - 2], 16)
                        prev1 = jnp.left_shift(words[depth - 1], 16)
                        for i in range(depth):
                            cur = words[i]
                            mixed = jnp.where(two, prev2, jnp.where(one, prev1, cur))
                            moved = jnp.take_along_axis(mixed, source, axis=1)
                            row = i * comps + c
                            acc[row] += weight * jnp.left_shift(moved, 16).astype(jnp.float32)
                            acc[row + half] += weight * moved.astype(jnp.float32)
                            prev2, prev1 = prev1, cur
            for r in range(rows):
                total[r, part, :] = acc[r]

    def send_sum(q):
        top = jnp.abs(total[0])
        for r in range(1, rows):
            top = jnp.maximum(top, jnp.abs(total[r]))
        top = jnp.maximum(jnp.max(top, axis=0, keepdims=True), 1e-30)
        top_out[q] = top * (1.0 / (TOP * 65536.0))
        inverse = jnp.broadcast_to(TOP / top, (variations, LANES))
        for r in range(half):
            low = lax.round(total[r] * inverse, nearest)
            high = lax.round(total[r + half] * inverse - low * (1.0 / 65536.0), nearest)
            sum_out[q, r] = jnp.left_shift(high.astype(jnp.int32), 16) + low.astype(jnp.int32)
        there = q * plane + i_own
        remote(sum_out.at[q], sum_in.at[z], send_p, recv_p.at[z], there).start()
        remote(top_out.at[q], top_in.at[z], send_p, recv_p.at[z], there).start()

    def sum_plane(ring, carry):
        q = plane_of(ring)

        @pl.when(inside(q))
        def _():
            @pl.when(q != z)
            def _():
                await_bytes(word_in.at[q], recv_w.at[q])

            spread(q)
            total[...] = jnp.zeros(total.shape, jnp.float32)

            def sources(t, carry):
                i_first = ((i_own // pair + t + 1) % (plane // pair)) * pair
                for d in range(pair):
                    @pl.when(i_first + d != i_own)
                    def _():
                        await_bytes(trace_bytes, recv_t.at[q * plane + i_first + d])

                add_traces(q, i_first)
                return carry

            lax.fori_loop(0, plane // pair, sources, 0)

            @pl.when(q != z)
            def _():
                send_sum(q)

            @pl.when(q == z)
            def _():
                motion[comps:comps + rows] = total[...]

        return carry

    lax.fori_loop(0, last_ring + 1, sum_plane, 0)

    def add_sum(t, carry):
        ring = jnp.bitwise_xor(t, 1)
        q = plane_of(ring)

        @pl.when(inside(q))
        def _():
            await_bytes(sum_bytes, recv_p.at[q])
            scale = jnp.broadcast_to(top_in[q], (variations, LANES))
            for r in range(half):
                word = sum_in[q, r]
                motion[comps + r] += jnp.left_shift(word, 16).astype(jnp.float32) * scale
                motion[comps + r + half] += word.astype(jnp.float32) * scale

        return carry

    lax.fori_loop(0, last_ring, add_sum, 0)

    for v in range(variations):
        lhs = jnp.concatenate([motion[comps:comps + rows, v, :], motion[0:rows, v, :]], axis=1)
        high = lhs.astype(jnp.bfloat16).astype(jnp.float32)
        pair_rows = jnp.concatenate([high, lhs - high], axis=0).astype(jnp.bfloat16)
        main = jnp.dot(pair_rows, high_taps[v], preferred_element_type=jnp.float32)
        minor = jnp.dot(pair_rows[:rows], low_taps[v], preferred_element_type=jnp.float32)
        out_ref[v] = main[:rows] + (main[rows:] + minor)

    others = pl.ds(0, n - 1)
    for ref, sem in ((want_v.at[others], send_m), (gain_v.at[others], send_m)):
        await_bytes(ref, sem)
    sent = pl.ds(0, planes * (plane - 1))
    if plane > 1:
        for ref in (box.at[sent], scale_box.at[sent]):
            await_bytes(ref, send_t)
    if planes > 1:
        far = pl.ds(0, planes - 1)
        await_bytes(word_in.at[far], send_w)
        for ref in (sum_in.at[far], top_in.at[far]):
            await_bytes(ref, send_p)


def local(plane, green_tensors, block_lists, block_count, onset_steps, slip_amount, mechanism, slip_rate):
    held, points, strains, comps, length = green_tensors.shape
    ruptures, listed = block_lists.shape
    assert ruptures == 1
    variations = onset_steps.shape[1]
    n = lax.axis_size("pts")
    cap = max(1, listed // n)
    tiles = length // LANES
    rows = tiles * comps
    planes = n // plane
    width = plane * cap * points
    fold = LANES // width
    assert listed * points <= LANES and rows == 16 and variations % 8 == 0
    assert fold * width == LANES and variations % fold == 0 and points & (points - 1) == 0
    green = green_tensors.reshape(held, points, strains, comps, tiles, LANES)
    green = green.transpose(0, 1, 2, 4, 3, 5).reshape(held, points, strains, rows, LANES)

    hbm = pl.BlockSpec(memory_space=pltpu.MemorySpace.HBM)
    vmem = pl.BlockSpec(memory_space=pltpu.VMEM)
    dma = pltpu.SemaphoreType.DMA
    i32, f32 = jnp.int32, jnp.float32
    seismograms = pl.pallas_call(
        functools.partial(seismogram_kernel, n, plane, cap, held, points, comps),
        out_shape=jax.ShapeDtypeStruct((variations, rows, LANES), f32),
        in_specs=[pl.BlockSpec(memory_space=pltpu.SMEM)] + [hbm] * 6,
        out_specs=vmem,
        scratch_shapes=[
            pltpu.VMEM((1, listed), i32),
            pltpu.VMEM((1, strains), f32),
            pltpu.VMEM((1, LANES), f32),
            pltpu.VMEM((held, points, strains, rows, LANES), jnp.bfloat16),
            pltpu.VMEM((variations, listed * points), i32),
            pltpu.VMEM((variations, listed * points), f32),
            pltpu.VMEM((variations, LANES), f32),
            pltpu.VMEM((n, cap, LANES), i32),
            pltpu.VMEM((n, cap, LANES), i32),
            pltpu.VMEM((n, 1, LANES), f32),
            pltpu.VMEM((planes, variations // fold, LANES), i32),
            pltpu.VMEM((planes, variations // fold, LANES), i32),
            pltpu.VMEM((2 * n, cap, points, rows // 2, LANES), i32),
            pltpu.VMEM((2 * n, 1, cap * LANES), f32),
            pltpu.VMEM((planes, rows // 2, variations, LANES), i32),
            pltpu.VMEM((planes, rows // 2, variations, LANES), i32),
            pltpu.VMEM((planes, 1, LANES), f32),
            pltpu.VMEM((planes, 1, LANES), f32),
            pltpu.VMEM((rows, variations, LANES), f32),
            pltpu.VMEM((rows + comps, variations, LANES), f32),
            pltpu.VMEM((variations, 2 * LANES, LANES), jnp.bfloat16),
            pltpu.VMEM((variations, 2 * LANES, LANES), jnp.bfloat16),
            pltpu.VMEM((width, variations, LANES), i32),
            pltpu.VMEM((width, variations, LANES), i32),
            pltpu.VMEM((width, variations, LANES), f32),
            pltpu.VMEM((plane * (cap + 1), 1, LANES), i32),
            pltpu.VMEM((cap * (points * rows // 2 + 1), 1, LANES), i32),
            pltpu.VMEM((rows // 2 * variations + 1, 1, LANES), i32),
            dma((6,)), pltpu.SemaphoreType.REGULAR((planes,)), dma, dma((planes,)), dma, dma((planes,)),
            dma, dma((n,)), dma, dma((planes,)),
        ],
        compiler_params=pltpu.CompilerParams(
            collective_id=0, has_side_effects=True, vmem_limit_bytes=32 << 20),
        name="seismograms",
    )(block_count, *(pltpu.with_memory_space_constraint(x, pltpu.MemorySpace.HBM) for x in (
        block_lists, mechanism, green, onset_steps[0], slip_amount[0], slip_rate[0])))
    out = seismograms.reshape(variations, tiles, comps, LANES).transpose(0, 2, 1, 3)
    return out.reshape(1, variations, comps, length)


def solution(mesh):
    n = mesh.shape["pts"]
    line = mesh.devices.reshape(-1, n)[0]
    heights = [getattr(d, "coords", (0, 0, 0))[2] for d in line]
    plane = sum(1 for h in heights if h == heights[0])
    assert n % plane == 0
    in_specs = (
        P(("site", "pts"), None, None, None, None),
        P(("site", "pts"), None),
        P(("site", "pts")),
        P(("site", "pts"), None, None),
        P(("site", "pts"), None, None),
        P(("site", "pts"), None),
        P(("site", "pts"), None, None),
    )
    out_specs = P(("site", "pts"), None, None, None)
    return jax.shard_map(functools.partial(local, plane), mesh=mesh, in_specs=in_specs, out_specs=out_specs,
                         check_vma=False)
```

```python
import functools

import jax
import jax.numpy as jnp
from jax import lax
from jax.experimental import pallas as pl
from jax.experimental.pallas import tpu as pltpu
from jax.sharding import PartitionSpec as P

LANES = 128
TOP = 32766.0


def seismogram_kernel(n, plane, cap, held, points, comps,
                      count_s, list_hbm, mech_hbm, green_hbm, onset_hbm, slip_hbm, rate_hbm, out_ref,
                      list_v, mech_v, mech_row, green, onset_v, slip_v, rate_v,
                      table, own_v, own_s, want_v, gain_v, outbox, out_scale, inbox, in_scale,
                      motion, high_taps, low_taps, source_of, back_of, weight_of, meta_bytes, trace_bytes,
                      local_sem, far_sem, send_m, recv_m, send_t, recv_t):
    me = lax.axis_index("pts")
    planes = n // plane
    z = me // plane
    i_own = me % plane
    toward = jnp.where(z < planes // 2, 1, -1)
    listed = list_hbm.shape[-1]
    strains = mech_hbm.shape[-1]
    variations, rows = out_ref.shape[0], out_ref.shape[1]
    tiles = rows // comps
    half = rows // 2
    mesh_id = pl.DeviceIdType.MESH

    barrier = pltpu.get_barrier_semaphore()

    def inside(q):
        return jnp.logical_and(q >= 0, q < planes)

    def in_plane(q, action):
        def body(t, carry):
            action(q * plane + (i_own + t) % plane)
            return carry

        @pl.when(inside(q))
        def _():
            lax.fori_loop(0, plane, body, 0, unroll=True)

    def beside(action):
        def body(t, carry):
            action(z * plane + (i_own + t) % plane)
            return carry

        lax.fori_loop(1, plane, body, 0, unroll=True)

    def greet(there):
        pl.semaphore_signal(barrier, inc=1, device_id={"pts": there}, device_id_type=mesh_id)

    local_copies = [
        pltpu.make_async_copy(src, dst, local_sem.at[i]) for i, (src, dst) in enumerate([
            (list_hbm, list_v), (mech_hbm, mech_v),
            (onset_hbm, onset_v), (slip_hbm, slip_v), (rate_hbm, rate_v), (green_hbm, green)])]
    for copy in local_copies:
        copy.start()
    in_plane(z + toward, greet)
    in_plane(z - toward, greet)
    beside(greet)

    for copy in local_copies[:2]:
        copy.wait()

    slots = n * cap

    def holder_of(blocks):
        if held & (held - 1) == 0:
            return jnp.right_shift(blocks, held.bit_length() - 1)
        return sum((blocks >= h * held).astype(jnp.int32) for h in range(1, n))

    k_across = lax.broadcasted_iota(jnp.int32, (listed, listed), 1)
    k_down = lax.broadcasted_iota(jnp.int32, (listed, listed), 0)
    as_row = jnp.broadcast_to(list_v[...], (listed, listed))
    as_col = jnp.sum(jnp.where(k_across == k_down, as_row, 0), axis=1, keepdims=True)
    holder_row = holder_of(as_row)
    holder_col = holder_of(as_col)
    same = holder_row == holder_col
    rank_row = jnp.sum(jnp.where(jnp.logical_and(same, k_down < k_across), 1, 0), axis=0, keepdims=True)
    rank_col = jnp.sum(jnp.where(jnp.logical_and(same, k_across < k_down), 1, 0), axis=1, keepdims=True)
    slot_down = lax.broadcasted_iota(jnp.int32, (slots, listed), 0)
    slot_row = holder_row[0:1] * cap + rank_row
    block_row = as_row[0:1] - holder_row[0:1] * held
    hit = slot_down == jnp.broadcast_to(slot_row, (slots, listed))
    block_col = jnp.sum(jnp.where(hit, jnp.broadcast_to(block_row, (slots, listed)), 0), axis=1, keepdims=True)
    block_col = jnp.broadcast_to(block_col, (slots, LANES))
    for h in range(n):
        table[h] = block_col[h * cap:(h + 1) * cap]
    mech_row[...] = jnp.zeros(mech_row.shape, jnp.float32)
    mech_row[:, 0:strains] = mech_v[...]

    has_low = jnp.where(z > 0, 1, 0)
    has_high = jnp.where(z < planes - 1, 1, 0)
    pl.semaphore_wait(barrier, plane - 1 + plane * (has_low + has_high))

    def remote(src, dst, send, recv, there):
        return pltpu.make_async_remote_copy(
            src_ref=src, dst_ref=dst, send_sem=send, recv_sem=recv,
            device_id={"pts": there}, device_id_type=mesh_id)

    def tell(k):
        for sign in (-1, 1):
            q = z + sign * k

            @pl.when(jnp.logical_and(inside(q), inside(z - sign)))
            def _():
                pl.semaphore_signal(far_sem.at[q], inc=1, device_id={"pts": me - sign * plane},
                                    device_id_type=mesh_id)

    def start_meta(there):
        remote(table.at[there], want_v.at[me], send_m, recv_m.at[z], there).start()
        remote(mech_row, gain_v.at[me], send_m, recv_m.at[z], there).start()

    def wait_meta(q):
        pltpu.make_async_copy(meta_bytes, meta_bytes, recv_m.at[q]).wait()

    def make_taps():
        i_row = lax.broadcasted_iota(jnp.int32, (LANES, LANES), 0)
        j_lane = lax.broadcasted_iota(jnp.int32, (LANES, LANES), 1)
        near_mask = j_lane >= i_row
        motion[...] = jnp.zeros(motion.shape, jnp.float32)

        def taps(v, carry):
            rate = jnp.broadcast_to(rate_v[pl.ds(v, 1), :], (LANES, LANES))
            turned = pltpu.roll(rate, 0, 1, stride=1, stride_axis=0)
            both = jnp.concatenate(
                [jnp.where(near_mask, turned, 0.0), jnp.where(near_mask, 0.0, turned)], axis=0)
            high = both.astype(jnp.bfloat16)
            high_taps[v] = high
            low_taps[v] = (both - high.astype(jnp.float32)).astype(jnp.bfloat16)
            return carry

        lax.fori_loop(0, variations, taps, 0, unroll=4)

    def spread_points():
        lane = lax.broadcasted_iota(jnp.int32, (variations, LANES), 1)
        count = count_s[0]
        onsets = onset_v[...]
        slips = slip_v[...]

        def spread(q, carry):
            pick = jnp.full((variations, LANES), q, jnp.int32)
            onset = jnp.take_along_axis(onsets, pick, axis=1)
            slip = jnp.take_along_axis(slips, pick, axis=1)
            shift = jnp.bitwise_and(onset, LANES - 1)
            source_of[q] = lane - shift
            back_of[q] = jnp.right_shift(onset, 7) + (lane >= LANES - shift).astype(jnp.int32)
            used = jnp.where(pick < count * points, 1.0, 0.0)
            weight_of[q] = slip * used
            return carry

        lax.fori_loop(0, listed * points, spread, 0, unroll=16)
        for p in range(points):
            source_of[listed * points + p] = lane
            back_of[listed * points + p] = jnp.zeros((variations, LANES), jnp.int32)
            weight_of[listed * points + p] = jnp.zeros((variations, LANES), jnp.float32)

    tell(1)
    in_plane(z + toward, start_meta)
    in_plane(z - toward, start_meta)

    def reach(k, carry):
        for sign in (-1, 1):
            q = z + sign * k

            @pl.when(inside(q))
            def _():
                pl.semaphore_wait(far_sem.at[q], 1)

        tell(k)
        in_plane(z + toward * k, start_meta)
        in_plane(z - toward * k, start_meta)
        return carry

    beside(start_meta)
    for copy in local_copies[4:5]:
        copy.wait()
    make_taps()
    if planes > 2:
        reach(2, 0)
    for copy in local_copies[2:4]:
        copy.wait()
    spread_points()
    lax.fori_loop(3, planes, reach, 0)

    as_k = lax.broadcasted_iota(jnp.int32, (listed, LANES), 0)
    lane_slot = lax.broadcasted_iota(jnp.int32, (listed, LANES), 1)
    mine = lane_slot == holder_col * cap + rank_col
    own_v[...] = jnp.sum(jnp.where(mine, as_k - listed, 0), axis=0, keepdims=True) + listed
    to_scalar = pltpu.make_async_copy(own_v, own_s, local_sem.at[6])
    to_scalar.start()
    local_copies[5].wait()

    def encode(wants, gains, box, scale_box, at):
        gain = [jnp.broadcast_to(gains[:, s:s + 1], (rows, LANES)) for s in range(strains)]
        lane_row = lax.broadcasted_iota(jnp.int32, (1, LANES), 1)
        scales = jnp.zeros((1, LANES), jnp.float32)
        for slot in range(cap):
            block = wants[slot, 0]
            traces = []
            for p in range(points):
                total = gain[0] * green[block, p, 0].astype(jnp.float32)
                for s in range(1, strains):
                    total += gain[s] * green[block, p, s].astype(jnp.float32)
                traces.append(total)
            top = jnp.abs(traces[0])
            for part in traces[1:]:
                top = jnp.maximum(top, jnp.abs(part))
            top = jnp.max(jnp.max(top, axis=0, keepdims=True), axis=1, keepdims=True)
            top = jnp.broadcast_to(jnp.maximum(top, 1e-30), (1, LANES))
            scales = jnp.where(lane_row >= slot * (LANES // cap), top * (1.0 / (TOP * 65536.0)), scales)
            inverse = jnp.broadcast_to(TOP / top, (half, LANES))
            for p in range(points):
                low = lax.round(traces[p][:half] * inverse, lax.RoundingMethod.TO_NEAREST_EVEN)
                high = lax.round(traces[p][half:] * inverse - low * (1.0 / 65536.0),
                                 lax.RoundingMethod.TO_NEAREST_EVEN)
                box[at, slot, p] = jnp.left_shift(high.astype(jnp.int32), 16) + low.astype(jnp.int32)
        scale_box[at] = scales

    def encode_to(there):
        encode(want_v[there], gain_v[there], outbox, out_scale, there)
        remote(outbox.at[there], inbox.at[me], send_t, recv_t.at[me // 2], there).start()
        remote(out_scale.at[there], in_scale.at[me], send_t, recv_t.at[me // 2], there).start()

    chip = plane // 2
    steps = 4 * planes - 2

    def encode_step(u, carry):
        middle = u >= 6
        k = jnp.where(middle, planes - 1 - (u - 6) // 4, jnp.where(u >= 4, 0, 1))
        away = jnp.where(middle, (u - 6) % 4 >= 2, jnp.logical_or(u == 1, u == 2))
        part = jnp.where(middle, (u - 6) % 2, jnp.logical_or(jnp.logical_or(u == 2, u == 3), u == 5).astype(jnp.int32))
        q = z + jnp.where(away, -toward, toward) * k

        @pl.when(inside(q))
        def _():
            @pl.when(jnp.logical_and(part == 0, k > 0))
            def _():
                wait_meta(q)

            @pl.when(jnp.logical_and(part == 0, k == 0))
            def _():
                beside_bytes = meta_bytes.at[pl.ds(0, (plane - 1) * (cap + 1))]
                pltpu.make_async_copy(beside_bytes, beside_bytes, recv_m.at[z]).wait()

            def one(t, carry):
                there = q * plane + (i_own // chip * chip + part * chip + t) % plane

                @pl.when(there != me)
                def _():
                    encode_to(there)

                return carry

            lax.fori_loop(0, chip, one, 0)

        return carry

    def encode_own():
        encode(table[me], mech_row[...], inbox, in_scale, me)

    depth = tiles // 2

    def add_traces(js):
        bases = [own_s[0, j * cap + slot] * points for j in js for slot in range(cap)]
        scales = [jnp.broadcast_to(in_scale[j][:, slot * (LANES // cap):slot * (LANES // cap) + 1], (8, LANES))
                  for j in js for slot in range(cap)]
        for group in range(variations // 8):
            part = slice(group * 8, group * 8 + 8)
            acc = [motion[comps + q, part, :] for q in range(rows)]
            for e, (base, scale) in enumerate(zip(bases, scales)):
                j, slot = js[e // cap], e % cap
                for p in range(points):
                    source = jnp.bitwise_and(source_of[base + p, part, :], LANES - 1)
                    back = back_of[base + p, part, :]
                    weight = weight_of[base + p, part, :] * scale
                    one = back >= 1
                    two = back >= 2
                    for c in range(comps):
                        words = [jnp.broadcast_to(
                            inbox[j, slot, p, i * comps + c:i * comps + c + 1, :], (8, LANES))
                            for i in range(depth)]
                        prev2 = jnp.left_shift(words[depth - 2], 16)
                        prev1 = jnp.left_shift(words[depth - 1], 16)
                        for i in range(depth):
                            cur = words[i]
                            mixed = jnp.where(two, prev2, jnp.where(one, prev1, cur))
                            moved = jnp.take_along_axis(mixed, source, axis=1)
                            row = i * comps + c
                            acc[row] += weight * jnp.left_shift(moved, 16).astype(jnp.float32)
                            acc[row + half] += weight * moved.astype(jnp.float32)
                            prev2, prev1 = prev1, cur
            for q in range(rows):
                motion[comps + q, part, :] = acc[q]

    def arrive(t, carry):
        ring = t // chip
        k = (ring + 1) // 2
        q = z + jnp.where(ring % 2 == 1, -toward, toward) * k
        first = q * plane + ((i_own // 2 + t) % chip) * 2

        @pl.when(inside(q))
        def _():
            @pl.when(first == me // 2 * 2)
            def _():
                mate = trace_bytes.at[pl.ds(0, cap * points * half + 1)]
                pltpu.make_async_copy(mate, mate, recv_t.at[first // 2]).wait()

            @pl.when(first != me // 2 * 2)
            def _():
                pltpu.make_async_copy(trace_bytes, trace_bytes, recv_t.at[first // 2]).wait()

            add_traces([first, first + 1])

        return carry

    lax.fori_loop(0, 6, encode_step, 0)
    encode_own()
    to_scalar.wait()
    early = jnp.where(inside(z + toward * (planes - 1)), chip, 0)
    lax.fori_loop(0, early, arrive, 0)
    lax.fori_loop(6, steps, encode_step, 0)
    lax.fori_loop(early, (2 * planes - 1) * chip, arrive, 0)

    for v in range(variations):
        lhs = jnp.concatenate([motion[comps:comps + rows, v, :], motion[0:rows, v, :]], axis=1)
        high = lhs.astype(jnp.bfloat16).astype(jnp.float32)
        pair = jnp.concatenate([high, lhs - high], axis=0).astype(jnp.bfloat16)
        main = jnp.dot(pair, high_taps[v], preferred_element_type=jnp.float32)
        minor = jnp.dot(pair[:rows], low_taps[v], preferred_element_type=jnp.float32)
        out_ref[v] = main[:rows] + (main[rows:] + minor)

    others = pl.ds(0, n - 1)
    for box, sem in ((want_v, send_m), (gain_v, send_m), (outbox, send_t), (out_scale, send_t)):
        pltpu.make_async_copy(box.at[others], box.at[others], sem).wait()


def local(plane, green_tensors, block_lists, block_count, onset_steps, slip_amount, mechanism, slip_rate):
    held, points, strains, comps, length = green_tensors.shape
    ruptures, listed = block_lists.shape
    assert ruptures == 1
    variations = onset_steps.shape[1]
    n = lax.axis_size("pts")
    cap = max(1, listed // n)
    tiles = length // LANES
    rows = tiles * comps
    assert n * cap <= LANES and listed * points <= LANES and rows == 16 and variations % 8 == 0
    green = green_tensors.reshape(held, points, strains, comps, tiles, LANES)
    green = green.transpose(0, 1, 2, 4, 3, 5).reshape(held, points, strains, rows, LANES)

    hbm = pl.BlockSpec(memory_space=pltpu.MemorySpace.HBM)
    vmem = pl.BlockSpec(memory_space=pltpu.VMEM)
    dma = pltpu.SemaphoreType.DMA
    planes = n // plane
    seismograms = pl.pallas_call(
        functools.partial(seismogram_kernel, n, plane, cap, held, points, comps),
        out_shape=jax.ShapeDtypeStruct((variations, rows, LANES), jnp.float32),
        in_specs=[pl.BlockSpec(memory_space=pltpu.SMEM)] + [hbm] * 6,
        out_specs=vmem,
        scratch_shapes=[
            pltpu.VMEM((1, listed), jnp.int32),
            pltpu.VMEM((1, strains), jnp.float32),
            pltpu.VMEM((1, LANES), jnp.float32),
            pltpu.VMEM((held, points, strains, rows, LANES), jnp.bfloat16),
            pltpu.VMEM((variations, listed * points), jnp.int32),
            pltpu.VMEM((variations, listed * points), jnp.float32),
            pltpu.VMEM((variations, LANES), jnp.float32),
            pltpu.VMEM((n, cap, LANES), jnp.int32),
            pltpu.VMEM((1, LANES), jnp.int32),
            pltpu.SMEM((1, LANES), jnp.int32),
            pltpu.VMEM((n, cap, LANES), jnp.int32),
            pltpu.VMEM((n, 1, LANES), jnp.float32),
            pltpu.VMEM((n, cap, points, rows // 2, LANES), jnp.int32),
            pltpu.VMEM((n, 1, LANES), jnp.float32),
            pltpu.VMEM((n, cap, points, rows // 2, LANES), jnp.int32),
            pltpu.VMEM((n, 1, LANES), jnp.float32),
            pltpu.VMEM((rows + comps, variations, LANES), jnp.float32),
            pltpu.VMEM((variations, 2 * LANES, LANES), jnp.bfloat16),
            pltpu.VMEM((variations, 2 * LANES, LANES), jnp.bfloat16),
            pltpu.VMEM(((listed + 1) * points, variations, LANES), jnp.int32),
            pltpu.VMEM(((listed + 1) * points, variations, LANES), jnp.int32),
            pltpu.VMEM(((listed + 1) * points, variations, LANES), jnp.float32),
            pltpu.VMEM((plane * (cap + 1), 1, LANES), jnp.int32),
            pltpu.VMEM((2 * (cap * points * rows // 2 + 1), 1, LANES), jnp.int32),
            dma((7,)), pltpu.SemaphoreType.REGULAR((planes,)), dma, dma((planes,)), dma, dma((n // 2,)),
        ],
        compiler_params=pltpu.CompilerParams(
            collective_id=0, has_side_effects=True, vmem_limit_bytes=32 << 20),
        name="seismograms",
    )(block_count, *(pltpu.with_memory_space_constraint(x, pltpu.MemorySpace.HBM) for x in (
        block_lists, mechanism, green, onset_steps[0], slip_amount[0], slip_rate[0])))
    out = seismograms.reshape(variations, tiles, comps, LANES).transpose(0, 2, 1, 3)
    return out.reshape(1, variations, comps, length)


def solution(mesh):
    n = mesh.shape["pts"]
    line = mesh.devices.reshape(-1, n)[0]
    heights = [getattr(d, "coords", (0, 0, 0))[2] for d in line]
    plane = sum(1 for h in heights if h == heights[0])
    assert n % plane == 0 and plane % 2 == 0
    in_specs = (
        P(("site", "pts"), None, None, None, None),
        P(("site", "pts"), None),
        P(("site", "pts")),
        P(("site", "pts"), None, None),
        P(("site", "pts"), None, None),
        P(("site", "pts"), None),
        P(("site", "pts"), None, None),
    )
    out_specs = P(("site", "pts"), None, None, None)
    return jax.shard_map(functools.partial(local, plane), mesh=mesh, in_specs=in_specs, out_specs=out_specs,
                         check_vma=False)
```

```python
import functools

import jax
import jax.numpy as jnp
from jax import lax
from jax.experimental import pallas as pl
from jax.experimental.pallas import tpu as pltpu
from jax.sharding import PartitionSpec as P

LANES = 128
TOP = 32766.0


def seismogram_kernel(n, plane, cap, held, points, comps,
                      count_s, list_hbm, mech_hbm, green_hbm, onset_hbm, slip_hbm, rate_hbm, out_ref,
                      list_v, mech_v, mech_row, green, onset_v, slip_v, rate_v,
                      table, own_v, own_s, want_v, gain_v, outbox, out_scale, inbox, in_scale,
                      motion, high_taps, low_taps, source_of, back_of, weight_of, meta_bytes, trace_bytes,
                      local_sem, far_sem, send_m, recv_m, send_t, recv_t):
    me = lax.axis_index("pts")
    planes = n // plane
    z = me // plane
    i_own = me % plane
    toward = jnp.where(z < planes // 2, 1, -1)
    listed = list_hbm.shape[-1]
    strains = mech_hbm.shape[-1]
    variations, rows = out_ref.shape[0], out_ref.shape[1]
    tiles = rows // comps
    half = rows // 2
    chip = plane // 2
    mesh_id = pl.DeviceIdType.MESH

    barrier = pltpu.get_barrier_semaphore()

    def inside(q):
        return jnp.logical_and(q >= 0, q < planes)

    def in_plane(q, action):
        def body(t, carry):
            action(q * plane + (i_own + t) % plane)
            return carry

        @pl.when(inside(q))
        def _():
            lax.fori_loop(0, plane, body, 0, unroll=True)

    def beside(action):
        def body(t, carry):
            action(z * plane + (i_own + t) % plane)
            return carry

        lax.fori_loop(1, plane, body, 0, unroll=True)

    def greet(there):
        pl.semaphore_signal(barrier, inc=1, device_id={"pts": there}, device_id_type=mesh_id)

    local_copies = [
        pltpu.make_async_copy(src, dst, local_sem.at[i]) for i, (src, dst) in enumerate([
            (list_hbm, list_v), (mech_hbm, mech_v),
            (onset_hbm, onset_v), (slip_hbm, slip_v), (rate_hbm, rate_v), (green_hbm, green)])]
    for copy in local_copies:
        copy.start()
    in_plane(z + toward, greet)
    in_plane(z - toward, greet)
    beside(greet)

    for copy in local_copies[:2]:
        copy.wait()

    slots = n * cap

    def holder_of(blocks):
        if held & (held - 1) == 0:
            return jnp.right_shift(blocks, held.bit_length() - 1)
        return sum((blocks >= h * held).astype(jnp.int32) for h in range(1, n))

    k_across = lax.broadcasted_iota(jnp.int32, (listed, listed), 1)
    k_down = lax.broadcasted_iota(jnp.int32, (listed, listed), 0)
    as_row = jnp.broadcast_to(list_v[...], (listed, listed))
    as_col = jnp.sum(jnp.where(k_across == k_down, as_row, 0), axis=1, keepdims=True)
    holder_row = holder_of(as_row)
    holder_col = holder_of(as_col)
    same = holder_row == holder_col
    rank_row = jnp.sum(jnp.where(jnp.logical_and(same, k_down < k_across), 1, 0), axis=0, keepdims=True)
    rank_col = jnp.sum(jnp.where(jnp.logical_and(same, k_across < k_down), 1, 0), axis=1, keepdims=True)
    slot_down = lax.broadcasted_iota(jnp.int32, (slots, listed), 0)
    slot_row = holder_row[0:1] * cap + rank_row
    block_row = as_row[0:1] - holder_row[0:1] * held
    hit = slot_down == jnp.broadcast_to(slot_row, (slots, listed))
    block_col = jnp.sum(jnp.where(hit, jnp.broadcast_to(block_row, (slots, listed)), 0), axis=1, keepdims=True)
    block_col = jnp.broadcast_to(block_col, (slots, LANES))
    for h in range(n):
        table[h] = block_col[h * cap:(h + 1) * cap]
    mech_row[...] = jnp.zeros(mech_row.shape, jnp.float32)
    mech_row[:, 0:strains] = mech_v[...]

    has_low = jnp.where(z > 0, 1, 0)
    has_high = jnp.where(z < planes - 1, 1, 0)
    pl.semaphore_wait(barrier, plane - 1 + plane * (has_low + has_high))

    def remote(src, dst, send, recv, there):
        return pltpu.make_async_remote_copy(
            src_ref=src, dst_ref=dst, send_sem=send, recv_sem=recv,
            device_id={"pts": there}, device_id_type=mesh_id)

    def tell(k):
        for sign in (-1, 1):
            q = z + sign * k

            @pl.when(jnp.logical_and(inside(q), inside(z - sign)))
            def _():
                pl.semaphore_signal(far_sem.at[q], inc=1, device_id={"pts": me - sign * plane},
                                    device_id_type=mesh_id)

    def start_meta(there):
        home = recv_m.at[2 * z + i_own // chip]
        remote(table.at[there], want_v.at[me], send_m, home, there).start()
        remote(mech_row, gain_v.at[me], send_m, home, there).start()

    def make_taps():
        i_row = lax.broadcasted_iota(jnp.int32, (LANES, LANES), 0)
        j_lane = lax.broadcasted_iota(jnp.int32, (LANES, LANES), 1)
        near_mask = j_lane >= i_row
        motion[...] = jnp.zeros(motion.shape, jnp.float32)

        def taps(v, carry):
            rate = jnp.broadcast_to(rate_v[pl.ds(v, 1), :], (LANES, LANES))
            turned = pltpu.roll(rate, 0, 1, stride=1, stride_axis=0)
            both = jnp.concatenate(
                [jnp.where(near_mask, turned, 0.0), jnp.where(near_mask, 0.0, turned)], axis=0)
            high = both.astype(jnp.bfloat16)
            high_taps[v] = high
            low_taps[v] = (both - high.astype(jnp.float32)).astype(jnp.bfloat16)
            return carry

        lax.fori_loop(0, variations, taps, 0, unroll=4)

    def spread_points():
        lane = lax.broadcasted_iota(jnp.int32, (variations, LANES), 1)
        count = count_s[0]
        onsets = onset_v[...]
        slips = slip_v[...]

        def spread(q, carry):
            pick = jnp.full((variations, LANES), q, jnp.int32)
            onset = jnp.take_along_axis(onsets, pick, axis=1)
            slip = jnp.take_along_axis(slips, pick, axis=1)
            shift = jnp.bitwise_and(onset, LANES - 1)
            source_of[q] = lane - shift
            back_of[q] = jnp.right_shift(onset, 7) + (lane >= LANES - shift).astype(jnp.int32)
            used = jnp.where(pick < count * points, 1.0, 0.0)
            weight_of[q] = slip * used
            return carry

        lax.fori_loop(0, listed * points, spread, 0, unroll=16)
        for p in range(points):
            source_of[listed * points + p] = lane
            back_of[listed * points + p] = jnp.zeros((variations, LANES), jnp.int32)
            weight_of[listed * points + p] = jnp.zeros((variations, LANES), jnp.float32)

    tell(1)
    in_plane(z + toward, start_meta)
    in_plane(z - toward, start_meta)

    def reach(k, carry):
        for sign in (-1, 1):
            q = z + sign * k

            @pl.when(inside(q))
            def _():
                pl.semaphore_wait(far_sem.at[q], 1)

        tell(k)
        in_plane(z + toward * k, start_meta)
        in_plane(z - toward * k, start_meta)
        return carry

    beside(start_meta)
    for copy in local_copies[4:5]:
        copy.wait()
    make_taps()
    if planes > 2:
        reach(2, 0)
    for copy in local_copies[2:4]:
        copy.wait()
    spread_points()
    lax.fori_loop(3, planes, reach, 0)

    as_k = lax.broadcasted_iota(jnp.int32, (listed, LANES), 0)
    lane_slot = lax.broadcasted_iota(jnp.int32, (listed, LANES), 1)
    mine = lane_slot == holder_col * cap + rank_col
    own_v[...] = jnp.sum(jnp.where(mine, as_k - listed, 0), axis=0, keepdims=True) + listed
    to_scalar = pltpu.make_async_copy(own_v, own_s, local_sem.at[6])
    to_scalar.start()
    local_copies[5].wait()

    def encode(wants, gains, box, scale_box, at):
        gain = [jnp.broadcast_to(gains[:, s:s + 1], (rows, LANES)) for s in range(strains)]
        lane_row = lax.broadcasted_iota(jnp.int32, (1, LANES), 1)
        scales = jnp.zeros((1, LANES), jnp.float32)
        for slot in range(cap):
            block = wants[slot, 0]
            traces = []
            for p in range(points):
                total = gain[0] * green[block, p, 0].astype(jnp.float32)
                for s in range(1, strains):
                    total += gain[s] * green[block, p, s].astype(jnp.float32)
                traces.append(total)
            top = jnp.abs(traces[0])
            for part in traces[1:]:
                top = jnp.maximum(top, jnp.abs(part))
            top = jnp.max(jnp.max(top, axis=0, keepdims=True), axis=1, keepdims=True)
            top = jnp.broadcast_to(jnp.maximum(top, 1e-30), (1, LANES))
            scales = jnp.where(lane_row >= slot * (LANES // cap), top * (1.0 / (TOP * 65536.0)), scales)
            inverse = jnp.broadcast_to(TOP / top, (half, LANES))
            for p in range(points):
                low = lax.round(traces[p][:half] * inverse, lax.RoundingMethod.TO_NEAREST_EVEN)
                high = lax.round(traces[p][half:] * inverse - low * (1.0 / 65536.0),
                                 lax.RoundingMethod.TO_NEAREST_EVEN)
                box[at, slot, p] = jnp.left_shift(high.astype(jnp.int32), 16) + low.astype(jnp.int32)
        scale_box[at] = scales

    def encode_to(there):
        encode(want_v[there], gain_v[there], outbox, out_scale, there)
        remote(outbox.at[there], inbox.at[me], send_t, recv_t.at[me // 2], there).start()
        remote(out_scale.at[there], in_scale.at[me], send_t, recv_t.at[me // 2], there).start()

    steps = 4 * planes - 2

    def encode_step(u, carry):
        middle = u >= 6
        w = (u - 6) // 2
        k = jnp.where(middle, planes - 1 - w // 2, jnp.where(u >= 4, 0, 1))
        away = jnp.where(middle, u % 2 == 1, jnp.logical_or(u == 1, u == 2))
        second = jnp.logical_or(jnp.logical_or(u == 2, u == 3), u == 5).astype(jnp.int32)
        part = jnp.where(middle, w % 2, second)
        q = z + jnp.where(away, -toward, toward) * k
        side = (i_own // chip + part) % 2

        @pl.when(inside(q))
        def _():
            @pl.when(k + part > 0)
            def _():
                pltpu.make_async_copy(meta_bytes, meta_bytes, recv_m.at[2 * q + side]).wait()

            if chip > 1:
                @pl.when(k + part == 0)
                def _():
                    mates = meta_bytes.at[pl.ds(0, (chip - 1) * (cap + 1))]
                    pltpu.make_async_copy(mates, mates, recv_m.at[2 * q + side]).wait()

            def one(t, carry):
                there = q * plane + side * chip + t

                @pl.when(there != me)
                def _():
                    encode_to(there)

                return carry

            lax.fori_loop(0, chip, one, 0)

        return carry

    def encode_own():
        encode(table[me], mech_row[...], inbox, in_scale, me)

    depth = tiles // 2

    def add_traces(js, groups):
        bases = [own_s[0, j * cap + slot] * points for j in js for slot in range(cap)]
        scales = [jnp.broadcast_to(in_scale[j][:, slot * (LANES // cap):slot * (LANES // cap) + 1], (8, LANES))
                  for j in js for slot in range(cap)]
        for group in groups:
            part = slice(group * 8, group * 8 + 8)
            acc = [motion[comps + q, part, :] for q in range(rows)]
            for e, (base, scale) in enumerate(zip(bases, scales)):
                j, slot = js[e // cap], e % cap
                for p in range(points):
                    source = jnp.bitwise_and(source_of[base + p, part, :], LANES - 1)
                    back = back_of[base + p, part, :]
                    weight = weight_of[base + p, part, :] * scale
                    one = back >= 1
                    two = back >= 2
                    for c in range(comps):
                        words = [jnp.broadcast_to(
                            inbox[j, slot, p, i * comps + c:i * comps + c + 1, :], (8, LANES))
                            for i in range(depth)]
                        prev2 = jnp.left_shift(words[depth - 2], 16)
                        prev1 = jnp.left_shift(words[depth - 1], 16)
                        for i in range(depth):
                            cur = words[i]
                            mixed = jnp.where(two, prev2, jnp.where(one, prev1, cur))
                            moved = jnp.take_along_axis(mixed, source, axis=1)
                            row = i * comps + c
                            acc[row] += weight * jnp.left_shift(moved, 16).astype(jnp.float32)
                            acc[row + half] += weight * moved.astype(jnp.float32)
                            prev2, prev1 = prev1, cur
            for q in range(rows):
                motion[comps + q, part, :] = acc[q]

    def sources(t):
        ring = t // chip
        k = (ring + 1) // 2
        q = z + jnp.where(ring % 2 == 1, -toward, toward) * k
        return q, q * plane + ((i_own // 2 + t) % chip) * 2

    def await_traces(first):
        @pl.when(first == me // 2 * 2)
        def _():
            mate = trace_bytes.at[pl.ds(0, cap * points * half + 1)]
            pltpu.make_async_copy(mate, mate, recv_t.at[first // 2]).wait()

        @pl.when(first != me // 2 * 2)
        def _():
            pltpu.make_async_copy(trace_bytes, trace_bytes, recv_t.at[first // 2]).wait()

    def arrive(t, carry):
        q, first = sources(t)

        @pl.when(inside(q))
        def _():
            await_traces(first)
            add_traces([first, first + 1], range(variations // 8))

        return carry

    def convolve(v):
        lhs = jnp.concatenate([motion[comps:comps + rows, v, :], motion[0:rows, v, :]], axis=1)
        high = lhs.astype(jnp.bfloat16).astype(jnp.float32)
        pair = jnp.concatenate([high, lhs - high], axis=0).astype(jnp.bfloat16)
        main = jnp.dot(pair, high_taps[v], preferred_element_type=jnp.float32)
        minor = jnp.dot(pair[:rows], low_taps[v], preferred_element_type=jnp.float32)
        out_ref[v] = main[:rows] + (main[rows:] + minor)

    lax.fori_loop(0, 6, encode_step, 0)
    encode_own()
    to_scalar.wait()
    early = jnp.where(inside(z + toward * (planes - 1)), chip, 0)
    lax.fori_loop(0, early, arrive, 0)
    lax.fori_loop(6, steps, encode_step, 0)
    last = 2 * jnp.where(toward > 0, planes - 1 - z, z) * chip + chip - 1
    lax.fori_loop(early, last, arrive, 0)
    _, first = sources(last)
    await_traces(first)
    for group in range(variations // 8):
        add_traces([first, first + 1], [group])
        for v in range(group * 8, group * 8 + 8):
            convolve(v)

    others = pl.ds(0, n - 1)
    for box, sem in ((want_v, send_m), (gain_v, send_m), (outbox, send_t), (out_scale, send_t)):
        pltpu.make_async_copy(box.at[others], box.at[others], sem).wait()


def local(plane, green_tensors, block_lists, block_count, onset_steps, slip_amount, mechanism, slip_rate):
    held, points, strains, comps, length = green_tensors.shape
    ruptures, listed = block_lists.shape
    assert ruptures == 1
    variations = onset_steps.shape[1]
    n = lax.axis_size("pts")
    cap = max(1, listed // n)
    tiles = length // LANES
    rows = tiles * comps
    assert n * cap <= LANES and listed * points <= LANES and rows == 16 and variations % 8 == 0
    green = green_tensors.reshape(held, points, strains, comps, tiles, LANES)
    green = green.transpose(0, 1, 2, 4, 3, 5).reshape(held, points, strains, rows, LANES)

    hbm = pl.BlockSpec(memory_space=pltpu.MemorySpace.HBM)
    vmem = pl.BlockSpec(memory_space=pltpu.VMEM)
    dma = pltpu.SemaphoreType.DMA
    planes = n // plane
    seismograms = pl.pallas_call(
        functools.partial(seismogram_kernel, n, plane, cap, held, points, comps),
        out_shape=jax.ShapeDtypeStruct((variations, rows, LANES), jnp.float32),
        in_specs=[pl.BlockSpec(memory_space=pltpu.SMEM)] + [hbm] * 6,
        out_specs=vmem,
        scratch_shapes=[
            pltpu.VMEM((1, listed), jnp.int32),
            pltpu.VMEM((1, strains), jnp.float32),
            pltpu.VMEM((1, LANES), jnp.float32),
            pltpu.VMEM((held, points, strains, rows, LANES), jnp.bfloat16),
            pltpu.VMEM((variations, listed * points), jnp.int32),
            pltpu.VMEM((variations, listed * points), jnp.float32),
            pltpu.VMEM((variations, LANES), jnp.float32),
            pltpu.VMEM((n, cap, LANES), jnp.int32),
            pltpu.VMEM((1, LANES), jnp.int32),
            pltpu.SMEM((1, LANES), jnp.int32),
            pltpu.VMEM((n, cap, LANES), jnp.int32),
            pltpu.VMEM((n, 1, LANES), jnp.float32),
            pltpu.VMEM((n, cap, points, rows // 2, LANES), jnp.int32),
            pltpu.VMEM((n, 1, LANES), jnp.float32),
            pltpu.VMEM((n, cap, points, rows // 2, LANES), jnp.int32),
            pltpu.VMEM((n, 1, LANES), jnp.float32),
            pltpu.VMEM((rows + comps, variations, LANES), jnp.float32),
            pltpu.VMEM((variations, 2 * LANES, LANES), jnp.bfloat16),
            pltpu.VMEM((variations, 2 * LANES, LANES), jnp.bfloat16),
            pltpu.VMEM(((listed + 1) * points, variations, LANES), jnp.int32),
            pltpu.VMEM(((listed + 1) * points, variations, LANES), jnp.int32),
            pltpu.VMEM(((listed + 1) * points, variations, LANES), jnp.float32),
            pltpu.VMEM((plane // 2 * (cap + 1), 1, LANES), jnp.int32),
            pltpu.VMEM((2 * (cap * points * rows // 2 + 1), 1, LANES), jnp.int32),
            dma((7,)), pltpu.SemaphoreType.REGULAR((planes,)), dma, dma((2 * planes,)), dma, dma((n // 2,)),
        ],
        compiler_params=pltpu.CompilerParams(
            collective_id=0, has_side_effects=True, vmem_limit_bytes=32 << 20),
        name="seismograms",
    )(block_count, *(pltpu.with_memory_space_constraint(x, pltpu.MemorySpace.HBM) for x in (
        block_lists, mechanism, green, onset_steps[0], slip_amount[0], slip_rate[0])))
    out = seismograms.reshape(variations, tiles, comps, LANES).transpose(0, 2, 1, 3)
    return out.reshape(1, variations, comps, length)


def solution(mesh):
    n = mesh.shape["pts"]
    line = mesh.devices.reshape(-1, n)[0]
    heights = [getattr(d, "coords", (0, 0, 0))[2] for d in line]
    plane = sum(1 for h in heights if h == heights[0])
    assert n % plane == 0 and plane % 2 == 0
    in_specs = (
        P(("site", "pts"), None, None, None, None),
        P(("site", "pts"), None),
        P(("site", "pts")),
        P(("site", "pts"), None, None),
        P(("site", "pts"), None, None),
        P(("site", "pts"), None),
        P(("site", "pts"), None, None),
    )
    out_specs = P(("site", "pts"), None, None, None)
    return jax.shard_map(functools.partial(local, plane), mesh=mesh, in_specs=in_specs, out_specs=out_specs,
                         check_vma=False)
```

```python
import functools

import jax
import jax.numpy as jnp
from jax import lax
from jax.experimental import pallas as pl
from jax.experimental.pallas import tpu as pltpu
from jax.sharding import PartitionSpec as P

LANES = 128
TOP = 32766.0


def seismogram_kernel(n, plane, cap, held, points, comps,
                      count_s, list_hbm, mech_hbm, green_hbm, onset_hbm, slip_hbm, rate_hbm, out_ref,
                      list_v, mech_v, mech_row, green, onset_v, slip_v, rate_v,
                      table, own_v, own_s, want_v, gain_v, outbox, out_scale, inbox, in_scale,
                      motion, high_taps, low_taps, source_of, back_of, weight_of, meta_bytes, trace_bytes,
                      local_sem, far_sem, send_m, recv_m, send_t, recv_t):
    me = lax.axis_index("pts")
    planes = n // plane
    z = me // plane
    i_own = me % plane
    toward = jnp.where(z < planes // 2, 1, -1)
    listed = list_hbm.shape[-1]
    strains = mech_hbm.shape[-1]
    variations, rows = out_ref.shape[0], out_ref.shape[1]
    tiles = rows // comps
    half = rows // 2
    chip = plane // 2
    mesh_id = pl.DeviceIdType.MESH

    barrier = pltpu.get_barrier_semaphore()

    def inside(q):
        return jnp.logical_and(q >= 0, q < planes)

    def in_plane(q, action):
        def body(t, carry):
            action(q * plane + (i_own + t) % plane)
            return carry

        @pl.when(inside(q))
        def _():
            lax.fori_loop(0, plane, body, 0, unroll=True)

    def beside(action):
        def body(t, carry):
            action(z * plane + (i_own + t) % plane)
            return carry

        lax.fori_loop(1, plane, body, 0, unroll=True)

    def greet(there):
        pl.semaphore_signal(barrier, inc=1, device_id={"pts": there}, device_id_type=mesh_id)

    local_copies = [
        pltpu.make_async_copy(src, dst, local_sem.at[i]) for i, (src, dst) in enumerate([
            (list_hbm, list_v), (mech_hbm, mech_v),
            (onset_hbm, onset_v), (slip_hbm, slip_v), (rate_hbm, rate_v), (green_hbm, green)])]
    for copy in local_copies:
        copy.start()
    in_plane(z + toward, greet)
    in_plane(z - toward, greet)
    beside(greet)

    for copy in local_copies[:2]:
        copy.wait()

    slots = n * cap

    def holder_of(blocks):
        if held & (held - 1) == 0:
            return jnp.right_shift(blocks, held.bit_length() - 1)
        return sum((blocks >= h * held).astype(jnp.int32) for h in range(1, n))

    k_across = lax.broadcasted_iota(jnp.int32, (listed, listed), 1)
    k_down = lax.broadcasted_iota(jnp.int32, (listed, listed), 0)
    as_row = jnp.broadcast_to(list_v[...], (listed, listed))
    as_col = jnp.sum(jnp.where(k_across == k_down, as_row, 0), axis=1, keepdims=True)
    holder_row = holder_of(as_row)
    holder_col = holder_of(as_col)
    same = holder_row == holder_col
    rank_row = jnp.sum(jnp.where(jnp.logical_and(same, k_down < k_across), 1, 0), axis=0, keepdims=True)
    rank_col = jnp.sum(jnp.where(jnp.logical_and(same, k_across < k_down), 1, 0), axis=1, keepdims=True)
    slot_down = lax.broadcasted_iota(jnp.int32, (slots, listed), 0)
    slot_row = holder_row[0:1] * cap + rank_row
    block_row = as_row[0:1] - holder_row[0:1] * held
    hit = slot_down == jnp.broadcast_to(slot_row, (slots, listed))
    block_col = jnp.sum(jnp.where(hit, jnp.broadcast_to(block_row, (slots, listed)), 0), axis=1, keepdims=True)
    block_col = jnp.broadcast_to(block_col, (slots, LANES))
    for h in range(n):
        table[h] = block_col[h * cap:(h + 1) * cap]
    mech_row[...] = jnp.zeros(mech_row.shape, jnp.float32)
    mech_row[:, 0:strains] = mech_v[...]

    has_low = jnp.where(z > 0, 1, 0)
    has_high = jnp.where(z < planes - 1, 1, 0)
    pl.semaphore_wait(barrier, plane - 1 + plane * (has_low + has_high))

    def remote(src, dst, send, recv, there):
        return pltpu.make_async_remote_copy(
            src_ref=src, dst_ref=dst, send_sem=send, recv_sem=recv,
            device_id={"pts": there}, device_id_type=mesh_id)

    def tell(k):
        for sign in (-1, 1):
            q = z + sign * k

            @pl.when(jnp.logical_and(inside(q), inside(z - sign)))
            def _():
                pl.semaphore_signal(far_sem.at[q], inc=1, device_id={"pts": me - sign * plane},
                                    device_id_type=mesh_id)

    def start_meta(there):
        home = recv_m.at[2 * z + i_own // chip]
        remote(table.at[there], want_v.at[me], send_m, home, there).start()
        remote(mech_row, gain_v.at[me], send_m, home, there).start()

    def make_taps():
        i_row = lax.broadcasted_iota(jnp.int32, (LANES, LANES), 0)
        j_lane = lax.broadcasted_iota(jnp.int32, (LANES, LANES), 1)
        near_mask = j_lane >= i_row
        motion[...] = jnp.zeros(motion.shape, jnp.float32)

        def taps(v, carry):
            rate = jnp.broadcast_to(rate_v[pl.ds(v, 1), :], (LANES, LANES))
            turned = pltpu.roll(rate, 0, 1, stride=1, stride_axis=0)
            both = jnp.concatenate(
                [jnp.where(near_mask, turned, 0.0), jnp.where(near_mask, 0.0, turned)], axis=0)
            high = both.astype(jnp.bfloat16)
            high_taps[v] = high
            low_taps[v] = (both - high.astype(jnp.float32)).astype(jnp.bfloat16)
            return carry

        lax.fori_loop(0, variations, taps, 0, unroll=4)

    def spread_points():
        lane = lax.broadcasted_iota(jnp.int32, (variations, LANES), 1)
        count = count_s[0]
        onsets = onset_v[...]
        slips = slip_v[...]

        def spread(q, carry):
            pick = jnp.full((variations, LANES), q, jnp.int32)
            onset = jnp.take_along_axis(onsets, pick, axis=1)
            slip = jnp.take_along_axis(slips, pick, axis=1)
            shift = jnp.bitwise_and(onset, LANES - 1)
            source_of[q] = lane - shift
            back_of[q] = jnp.right_shift(onset, 7) + (lane >= LANES - shift).astype(jnp.int32)
            used = jnp.where(pick < count * points, 1.0, 0.0)
            weight_of[q] = slip * used
            return carry

        lax.fori_loop(0, listed * points, spread, 0, unroll=16)
        for p in range(points):
            source_of[listed * points + p] = lane
            back_of[listed * points + p] = jnp.zeros((variations, LANES), jnp.int32)
            weight_of[listed * points + p] = jnp.zeros((variations, LANES), jnp.float32)

    tell(1)
    in_plane(z + toward, start_meta)
    in_plane(z - toward, start_meta)

    def reach(k, carry):
        for sign in (-1, 1):
            q = z + sign * k

            @pl.when(inside(q))
            def _():
                pl.semaphore_wait(far_sem.at[q], 1)

        tell(k)
        in_plane(z + toward * k, start_meta)
        in_plane(z - toward * k, start_meta)
        return carry

    beside(start_meta)
    for copy in local_copies[4:5]:
        copy.wait()
    make_taps()
    if planes > 2:
        reach(2, 0)
    for copy in local_copies[2:4]:
        copy.wait()
    spread_points()
    lax.fori_loop(3, planes, reach, 0)

    as_k = lax.broadcasted_iota(jnp.int32, (listed, LANES), 0)
    lane_slot = lax.broadcasted_iota(jnp.int32, (listed, LANES), 1)
    mine = lane_slot == holder_col * cap + rank_col
    own_v[...] = jnp.sum(jnp.where(mine, as_k - listed, 0), axis=0, keepdims=True) + listed
    to_scalar = pltpu.make_async_copy(own_v, own_s, local_sem.at[6])
    to_scalar.start()
    local_copies[5].wait()

    def encode(wants, gains, box, scale_box, at):
        gain = [jnp.broadcast_to(gains[:, s:s + 1], (rows, LANES)) for s in range(strains)]
        lane_row = lax.broadcasted_iota(jnp.int32, (1, LANES), 1)
        scales = jnp.zeros((1, LANES), jnp.float32)
        for slot in range(cap):
            block = wants[slot, 0]
            traces = []
            for p in range(points):
                total = gain[0] * green[block, p, 0].astype(jnp.float32)
                for s in range(1, strains):
                    total += gain[s] * green[block, p, s].astype(jnp.float32)
                traces.append(total)
            top = jnp.abs(traces[0])
            for part in traces[1:]:
                top = jnp.maximum(top, jnp.abs(part))
            top = jnp.max(jnp.max(top, axis=0, keepdims=True), axis=1, keepdims=True)
            top = jnp.broadcast_to(jnp.maximum(top, 1e-30), (1, LANES))
            scales = jnp.where(lane_row >= slot * (LANES // cap), top * (1.0 / (TOP * 65536.0)), scales)
            inverse = jnp.broadcast_to(TOP / top, (half, LANES))
            for p in range(points):
                low = lax.round(traces[p][:half] * inverse, lax.RoundingMethod.TO_NEAREST_EVEN)
                high = lax.round(traces[p][half:] * inverse - low * (1.0 / 65536.0),
                                 lax.RoundingMethod.TO_NEAREST_EVEN)
                box[at, slot, p] = jnp.left_shift(high.astype(jnp.int32), 16) + low.astype(jnp.int32)
        scale_box[at] = scales

    def encode_to(there):
        encode(want_v[there], gain_v[there], outbox, out_scale, there)
        remote(outbox.at[there], inbox.at[me], send_t, recv_t.at[me // 2], there).start()
        remote(out_scale.at[there], in_scale.at[me], send_t, recv_t.at[me // 2], there).start()

    steps = 4 * planes - 2

    def encode_step(u, carry):
        middle = u >= 6
        w = (u - 6) // 2
        k = jnp.where(middle, planes - 1 - w // 2, jnp.where(u >= 4, 0, 1))
        away = jnp.where(middle, u % 2 == 1, jnp.logical_or(u == 1, u == 2))
        second = jnp.logical_or(jnp.logical_or(u == 2, u == 3), u == 5).astype(jnp.int32)
        part = jnp.where(middle, w % 2, second)
        q = z + jnp.where(away, -toward, toward) * k
        side = (i_own // chip + part) % 2

        @pl.when(inside(q))
        def _():
            @pl.when(k + part > 0)
            def _():
                pltpu.make_async_copy(meta_bytes, meta_bytes, recv_m.at[2 * q + side]).wait()

            if chip > 1:
                @pl.when(k + part == 0)
                def _():
                    mates = meta_bytes.at[pl.ds(0, (chip - 1) * (cap + 1))]
                    pltpu.make_async_copy(mates, mates, recv_m.at[2 * q + side]).wait()

            def one(t, carry):
                there = q * plane + side * chip + jnp.where(k == 1, (t + i_own) % chip, t)

                @pl.when(there != me)
                def _():
                    encode_to(there)

                return carry

            lax.fori_loop(0, chip, one, 0)

        return carry

    def encode_own():
        encode(table[me], mech_row[...], inbox, in_scale, me)

    depth = tiles // 2

    def add_traces(js, groups):
        bases = [own_s[0, j * cap + slot] * points for j in js for slot in range(cap)]
        scales = [jnp.broadcast_to(in_scale[j][:, slot * (LANES // cap):slot * (LANES // cap) + 1], (8, LANES))
                  for j in js for slot in range(cap)]
        for group in groups:
            part = slice(group * 8, group * 8 + 8)
            acc = [motion[comps + q, part, :] for q in range(rows)]
            for e, (base, scale) in enumerate(zip(bases, scales)):
                j, slot = js[e // cap], e % cap
                for p in range(points):
                    source = jnp.bitwise_and(source_of[base + p, part, :], LANES - 1)
                    back = back_of[base + p, part, :]
                    weight = weight_of[base + p, part, :] * scale
                    one = back >= 1
                    two = back >= 2
                    for c in range(comps):
                        words = [jnp.broadcast_to(
                            inbox[j, slot, p, i * comps + c:i * comps + c + 1, :], (8, LANES))
                            for i in range(depth)]
                        prev2 = jnp.left_shift(words[depth - 2], 16)
                        prev1 = jnp.left_shift(words[depth - 1], 16)
                        for i in range(depth):
                            cur = words[i]
                            mixed = jnp.where(two, prev2, jnp.where(one, prev1, cur))
                            moved = jnp.take_along_axis(mixed, source, axis=1)
                            row = i * comps + c
                            acc[row] += weight * jnp.left_shift(moved, 16).astype(jnp.float32)
                            acc[row + half] += weight * moved.astype(jnp.float32)
                            prev2, prev1 = prev1, cur
            for q in range(rows):
                motion[comps + q, part, :] = acc[q]

    def sources(t):
        ring = t // chip
        k = (ring + 1) // 2
        q = z + jnp.where(ring % 2 == 1, -toward, toward) * k
        return q, q * plane + ((i_own // 2 + t) % chip) * 2

    def await_traces(first):
        @pl.when(first == me // 2 * 2)
        def _():
            mate = trace_bytes.at[pl.ds(0, cap * points * half + 1)]
            pltpu.make_async_copy(mate, mate, recv_t.at[first // 2]).wait()

        @pl.when(first != me // 2 * 2)
        def _():
            pltpu.make_async_copy(trace_bytes, trace_bytes, recv_t.at[first // 2]).wait()

    def arrive(t, carry):
        q, first = sources(t)

        @pl.when(inside(q))
        def _():
            await_traces(first)
            add_traces([first, first + 1], range(variations // 8))

        return carry

    def convolve(v):
        lhs = jnp.concatenate([motion[comps:comps + rows, v, :], motion[0:rows, v, :]], axis=1)
        high = lhs.astype(jnp.bfloat16).astype(jnp.float32)
        pair = jnp.concatenate([high, lhs - high], axis=0).astype(jnp.bfloat16)
        main = jnp.dot(pair, high_taps[v], preferred_element_type=jnp.float32)
        minor = jnp.dot(pair[:rows], low_taps[v], preferred_element_type=jnp.float32)
        out_ref[v] = main[:rows] + (main[rows:] + minor)

    lax.fori_loop(0, 6, encode_step, 0)
    encode_own()
    to_scalar.wait()
    early = jnp.where(inside(z + toward * (planes - 1)), chip, 0)
    lax.fori_loop(0, early, arrive, 0)
    lax.fori_loop(6, steps, encode_step, 0)
    last = 2 * jnp.where(toward > 0, planes - 1 - z, z) * chip + chip - 1
    lax.fori_loop(early, last, arrive, 0)
    _, first = sources(last)
    await_traces(first)
    for group in range(variations // 8):
        add_traces([first, first + 1], [group])
        for v in range(group * 8, group * 8 + 8):
            convolve(v)

    others = pl.ds(0, n - 1)
    for box, sem in ((want_v, send_m), (gain_v, send_m), (outbox, send_t), (out_scale, send_t)):
        pltpu.make_async_copy(box.at[others], box.at[others], sem).wait()


def local(plane, green_tensors, block_lists, block_count, onset_steps, slip_amount, mechanism, slip_rate):
    held, points, strains, comps, length = green_tensors.shape
    ruptures, listed = block_lists.shape
    assert ruptures == 1
    variations = onset_steps.shape[1]
    n = lax.axis_size("pts")
    cap = max(1, listed // n)
    tiles = length // LANES
    rows = tiles * comps
    assert n * cap <= LANES and listed * points <= LANES and rows == 16 and variations % 8 == 0
    green = green_tensors.reshape(held, points, strains, comps, tiles, LANES)
    green = green.transpose(0, 1, 2, 4, 3, 5).reshape(held, points, strains, rows, LANES)

    hbm = pl.BlockSpec(memory_space=pltpu.MemorySpace.HBM)
    vmem = pl.BlockSpec(memory_space=pltpu.VMEM)
    dma = pltpu.SemaphoreType.DMA
    planes = n // plane
    seismograms = pl.pallas_call(
        functools.partial(seismogram_kernel, n, plane, cap, held, points, comps),
        out_shape=jax.ShapeDtypeStruct((variations, rows, LANES), jnp.float32),
        in_specs=[pl.BlockSpec(memory_space=pltpu.SMEM)] + [hbm] * 6,
        out_specs=vmem,
        scratch_shapes=[
            pltpu.VMEM((1, listed), jnp.int32),
            pltpu.VMEM((1, strains), jnp.float32),
            pltpu.VMEM((1, LANES), jnp.float32),
            pltpu.VMEM((held, points, strains, rows, LANES), jnp.bfloat16),
            pltpu.VMEM((variations, listed * points), jnp.int32),
            pltpu.VMEM((variations, listed * points), jnp.float32),
            pltpu.VMEM((variations, LANES), jnp.float32),
            pltpu.VMEM((n, cap, LANES), jnp.int32),
            pltpu.VMEM((1, LANES), jnp.int32),
            pltpu.SMEM((1, LANES), jnp.int32),
            pltpu.VMEM((n, cap, LANES), jnp.int32),
            pltpu.VMEM((n, 1, LANES), jnp.float32),
            pltpu.VMEM((n, cap, points, rows // 2, LANES), jnp.int32),
            pltpu.VMEM((n, 1, LANES), jnp.float32),
            pltpu.VMEM((n, cap, points, rows // 2, LANES), jnp.int32),
            pltpu.VMEM((n, 1, LANES), jnp.float32),
            pltpu.VMEM((rows + comps, variations, LANES), jnp.float32),
            pltpu.VMEM((variations, 2 * LANES, LANES), jnp.bfloat16),
            pltpu.VMEM((variations, 2 * LANES, LANES), jnp.bfloat16),
            pltpu.VMEM(((listed + 1) * points, variations, LANES), jnp.int32),
            pltpu.VMEM(((listed + 1) * points, variations, LANES), jnp.int32),
            pltpu.VMEM(((listed + 1) * points, variations, LANES), jnp.float32),
            pltpu.VMEM((plane // 2 * (cap + 1), 1, LANES), jnp.int32),
            pltpu.VMEM((2 * (cap * points * rows // 2 + 1), 1, LANES), jnp.int32),
            dma((7,)), pltpu.SemaphoreType.REGULAR((planes,)), dma, dma((2 * planes,)), dma, dma((n // 2,)),
        ],
        compiler_params=pltpu.CompilerParams(
            collective_id=0, has_side_effects=True, vmem_limit_bytes=32 << 20),
        name="seismograms",
    )(block_count, *(pltpu.with_memory_space_constraint(x, pltpu.MemorySpace.HBM) for x in (
        block_lists, mechanism, green, onset_steps[0], slip_amount[0], slip_rate[0])))
    out = seismograms.reshape(variations, tiles, comps, LANES).transpose(0, 2, 1, 3)
    return out.reshape(1, variations, comps, length)


def solution(mesh):
    n = mesh.shape["pts"]
    line = mesh.devices.reshape(-1, n)[0]
    heights = [getattr(d, "coords", (0, 0, 0))[2] for d in line]
    plane = sum(1 for h in heights if h == heights[0])
    assert n % plane == 0 and plane % 2 == 0
    in_specs = (
        P(("site", "pts"), None, None, None, None),
        P(("site", "pts"), None),
        P(("site", "pts")),
        P(("site", "pts"), None, None),
        P(("site", "pts"), None, None),
        P(("site", "pts"), None),
        P(("site", "pts"), None, None),
    )
    out_specs = P(("site", "pts"), None, None, None)
    return jax.shard_map(functools.partial(local, plane), mesh=mesh, in_specs=in_specs, out_specs=out_specs,
                         check_vma=False)
```

```python
import functools

import jax
import jax.numpy as jnp
from jax import lax
from jax.experimental import pallas as pl
from jax.experimental.pallas import tpu as pltpu
from jax.sharding import PartitionSpec as P

LANES = 128
TOP = 32766.0


def seismogram_kernel(n, plane, cap, held, points, comps,
                      count_s, list_hbm, mech_hbm, green_hbm, onset_hbm, slip_hbm, rate_hbm, out_ref,
                      list_v, mech_v, mech_row, green, onset_v, slip_v, rate_v,
                      table, own_v, own_s, want_v, gain_v, outbox, out_scale, inbox, in_scale,
                      motion, high_taps, low_taps, source_of, back_of, weight_of, meta_bytes, trace_bytes,
                      local_sem, far_sem, send_m, recv_m, send_t, recv_t):
    me = lax.axis_index("pts")
    planes = n // plane
    z = me // plane
    i_own = me % plane
    toward = jnp.where(z < planes // 2, 1, -1)
    listed = list_hbm.shape[-1]
    strains = mech_hbm.shape[-1]
    variations, rows = out_ref.shape[0], out_ref.shape[1]
    tiles = rows // comps
    half = rows // 2
    chip = plane // 2
    mesh_id = pl.DeviceIdType.MESH

    barrier = pltpu.get_barrier_semaphore()

    def inside(q):
        return jnp.logical_and(q >= 0, q < planes)

    def in_plane(q, action):
        def body(t, carry):
            action(q * plane + (i_own + t) % plane)
            return carry

        @pl.when(inside(q))
        def _():
            lax.fori_loop(0, plane, body, 0, unroll=True)

    def beside(action):
        def body(t, carry):
            action(z * plane + (i_own + t) % plane)
            return carry

        lax.fori_loop(1, plane, body, 0, unroll=True)

    def greet(there):
        pl.semaphore_signal(barrier, inc=1, device_id={"pts": there}, device_id_type=mesh_id)

    local_copies = [
        pltpu.make_async_copy(src, dst, local_sem.at[i]) for i, (src, dst) in enumerate([
            (list_hbm, list_v), (mech_hbm, mech_v),
            (onset_hbm, onset_v), (slip_hbm, slip_v), (rate_hbm, rate_v), (green_hbm, green)])]
    for copy in local_copies:
        copy.start()
    in_plane(z + toward, greet)
    in_plane(z - toward, greet)
    beside(greet)

    for copy in local_copies[:2]:
        copy.wait()

    slots = n * cap

    def holder_of(blocks):
        if held & (held - 1) == 0:
            return jnp.right_shift(blocks, held.bit_length() - 1)
        return sum((blocks >= h * held).astype(jnp.int32) for h in range(1, n))

    k_across = lax.broadcasted_iota(jnp.int32, (listed, listed), 1)
    k_down = lax.broadcasted_iota(jnp.int32, (listed, listed), 0)
    as_row = jnp.broadcast_to(list_v[...], (listed, listed))
    as_col = jnp.sum(jnp.where(k_across == k_down, as_row, 0), axis=1, keepdims=True)
    holder_row = holder_of(as_row)
    holder_col = holder_of(as_col)
    same = holder_row == holder_col
    rank_row = jnp.sum(jnp.where(jnp.logical_and(same, k_down < k_across), 1, 0), axis=0, keepdims=True)
    rank_col = jnp.sum(jnp.where(jnp.logical_and(same, k_across < k_down), 1, 0), axis=1, keepdims=True)
    slot_down = lax.broadcasted_iota(jnp.int32, (slots, listed), 0)
    slot_row = holder_row[0:1] * cap + rank_row
    block_row = as_row[0:1] - holder_row[0:1] * held
    hit = slot_down == jnp.broadcast_to(slot_row, (slots, listed))
    block_col = jnp.sum(jnp.where(hit, jnp.broadcast_to(block_row, (slots, listed)), 0), axis=1, keepdims=True)
    block_col = jnp.broadcast_to(block_col, (slots, LANES))
    for h in range(n):
        table[h] = block_col[h * cap:(h + 1) * cap]
    mech_row[...] = jnp.zeros(mech_row.shape, jnp.float32)
    mech_row[:, 0:strains] = mech_v[...]

    has_low = jnp.where(z > 0, 1, 0)
    has_high = jnp.where(z < planes - 1, 1, 0)
    pl.semaphore_wait(barrier, plane - 1 + plane * (has_low + has_high))

    def remote(src, dst, send, recv, there):
        return pltpu.make_async_remote_copy(
            src_ref=src, dst_ref=dst, send_sem=send, recv_sem=recv,
            device_id={"pts": there}, device_id_type=mesh_id)

    def tell(k):
        for sign in (-1, 1):
            q = z + sign * k

            @pl.when(jnp.logical_and(inside(q), inside(z - sign)))
            def _():
                pl.semaphore_signal(far_sem.at[q], inc=1, device_id={"pts": me - sign * plane},
                                    device_id_type=mesh_id)

    def start_meta(there):
        home = recv_m.at[2 * z + i_own // chip]
        remote(table.at[there], want_v.at[me], send_m, home, there).start()
        remote(mech_row, gain_v.at[me], send_m, home, there).start()

    def make_taps():
        i_row = lax.broadcasted_iota(jnp.int32, (LANES, LANES), 0)
        j_lane = lax.broadcasted_iota(jnp.int32, (LANES, LANES), 1)
        near_mask = j_lane >= i_row
        motion[...] = jnp.zeros(motion.shape, jnp.float32)

        def taps(v, carry):
            rate = jnp.broadcast_to(rate_v[pl.ds(v, 1), :], (LANES, LANES))
            turned = pltpu.roll(rate, 0, 1, stride=1, stride_axis=0)
            both = jnp.concatenate(
                [jnp.where(near_mask, turned, 0.0), jnp.where(near_mask, 0.0, turned)], axis=0)
            high = both.astype(jnp.bfloat16)
            high_taps[v] = high
            low_taps[v] = (both - high.astype(jnp.float32)).astype(jnp.bfloat16)
            return carry

        lax.fori_loop(0, variations, taps, 0, unroll=4)

    def spread_points():
        lane = lax.broadcasted_iota(jnp.int32, (variations, LANES), 1)
        count = count_s[0]
        onsets = onset_v[...]
        slips = slip_v[...]

        def spread(q, carry):
            pick = jnp.full((variations, LANES), q, jnp.int32)
            onset = jnp.take_along_axis(onsets, pick, axis=1)
            slip = jnp.take_along_axis(slips, pick, axis=1)
            shift = jnp.bitwise_and(onset, LANES - 1)
            source_of[q] = lane - shift
            back_of[q] = jnp.right_shift(onset, 7) + (lane >= LANES - shift).astype(jnp.int32)
            used = jnp.where(pick < count * points, 1.0, 0.0)
            weight_of[q] = slip * used
            return carry

        lax.fori_loop(0, listed * points, spread, 0, unroll=16)
        for p in range(points):
            source_of[listed * points + p] = lane
            back_of[listed * points + p] = jnp.zeros((variations, LANES), jnp.int32)
            weight_of[listed * points + p] = jnp.zeros((variations, LANES), jnp.float32)

    tell(1)
    in_plane(z + toward, start_meta)
    in_plane(z - toward, start_meta)

    def reach(k, carry):
        for sign in (-1, 1):
            q = z + sign * k

            @pl.when(inside(q))
            def _():
                pl.semaphore_wait(far_sem.at[q], 1)

        tell(k)
        in_plane(z + toward * k, start_meta)
        in_plane(z - toward * k, start_meta)
        return carry

    beside(start_meta)
    for copy in local_copies[4:5]:
        copy.wait()
    make_taps()
    if planes > 2:
        reach(2, 0)
    for copy in local_copies[2:4]:
        copy.wait()
    spread_points()
    lax.fori_loop(3, planes, reach, 0)

    as_k = lax.broadcasted_iota(jnp.int32, (listed, LANES), 0)
    lane_slot = lax.broadcasted_iota(jnp.int32, (listed, LANES), 1)
    mine = lane_slot == holder_col * cap + rank_col
    own_v[...] = jnp.sum(jnp.where(mine, as_k - listed, 0), axis=0, keepdims=True) + listed
    to_scalar = pltpu.make_async_copy(own_v, own_s, local_sem.at[6])
    to_scalar.start()
    local_copies[5].wait()

    def encode(wants, gains, box, scale_box, at):
        gain = [jnp.broadcast_to(gains[:, s:s + 1], (rows, LANES)) for s in range(strains)]
        lane_row = lax.broadcasted_iota(jnp.int32, (1, LANES), 1)
        scales = jnp.zeros((1, LANES), jnp.float32)
        for slot in range(cap):
            block = wants[slot, 0]
            traces = []
            for p in range(points):
                total = gain[0] * green[block, p, 0].astype(jnp.float32)
                for s in range(1, strains):
                    total += gain[s] * green[block, p, s].astype(jnp.float32)
                traces.append(total)
            top = jnp.abs(traces[0])
            for part in traces[1:]:
                top = jnp.maximum(top, jnp.abs(part))
            top = jnp.max(jnp.max(top, axis=0, keepdims=True), axis=1, keepdims=True)
            top = jnp.broadcast_to(jnp.maximum(top, 1e-30), (1, LANES))
            scales = jnp.where(lane_row >= slot * (LANES // cap), top * (1.0 / (TOP * 65536.0)), scales)
            inverse = jnp.broadcast_to(TOP / top, (half, LANES))
            for p in range(points):
                low = lax.round(traces[p][:half] * inverse, lax.RoundingMethod.TO_NEAREST_EVEN)
                high = lax.round(traces[p][half:] * inverse - low * (1.0 / 65536.0),
                                 lax.RoundingMethod.TO_NEAREST_EVEN)
                box[at, slot, p] = jnp.left_shift(high.astype(jnp.int32), 16) + low.astype(jnp.int32)
        scale_box[at] = scales

    def encode_to(there):
        encode(want_v[there], gain_v[there], outbox, out_scale, there)
        remote(outbox.at[there], inbox.at[me], send_t, recv_t.at[me // 2], there).start()
        remote(out_scale.at[there], in_scale.at[me], send_t, recv_t.at[me // 2], there).start()

    steps = 4 * planes - 2

    def encode_step(u, carry):
        middle = u >= 6
        w = (u - 6) // 2
        k = jnp.where(middle, planes - 1 - w // 2, jnp.where(u >= 4, 0, 1))
        away = jnp.where(middle, u % 2 == 1, jnp.logical_or(u == 1, u == 2))
        second = jnp.logical_or(jnp.logical_or(u == 2, u == 3), u == 5).astype(jnp.int32)
        part = jnp.where(middle, w % 2, second)
        q = z + jnp.where(away, -toward, toward) * k
        side = (i_own // chip + part) % 2

        @pl.when(inside(q))
        def _():
            @pl.when(k + part > 0)
            def _():
                pltpu.make_async_copy(meta_bytes, meta_bytes, recv_m.at[2 * q + side]).wait()

            if chip > 1:
                @pl.when(k + part == 0)
                def _():
                    mates = meta_bytes.at[pl.ds(0, (chip - 1) * (cap + 1))]
                    pltpu.make_async_copy(mates, mates, recv_m.at[2 * q + side]).wait()

            def one(t, carry):
                there = q * plane + side * chip + jnp.where(k == 1, (t + i_own) % chip, t)

                @pl.when(there != me)
                def _():
                    encode_to(there)

                return carry

            lax.fori_loop(0, chip, one, 0)

        return carry

    def encode_own():
        encode(table[me], mech_row[...], inbox, in_scale, me)

    depth = tiles // 2

    def add_traces(js, groups):
        bases = [own_s[0, j * cap + slot] * points for j in js for slot in range(cap)]
        scales = [jnp.broadcast_to(in_scale[j][:, slot * (LANES // cap):slot * (LANES // cap) + 1], (8, LANES))
                  for j in js for slot in range(cap)]
        for group in groups:
            part = slice(group * 8, group * 8 + 8)
            acc = [motion[comps + q, part, :] for q in range(rows)]
            for e, (base, scale) in enumerate(zip(bases, scales)):
                j, slot = js[e // cap], e % cap
                for p in range(points):
                    source = jnp.bitwise_and(source_of[base + p, part, :], LANES - 1)
                    back = back_of[base + p, part, :]
                    weight = weight_of[base + p, part, :] * scale
                    one = back >= 1
                    two = back >= 2
                    for c in range(comps):
                        words = [jnp.broadcast_to(
                            inbox[j, slot, p, i * comps + c:i * comps + c + 1, :], (8, LANES))
                            for i in range(depth)]
                        prev2 = jnp.left_shift(words[depth - 2], 16)
                        prev1 = jnp.left_shift(words[depth - 1], 16)
                        for i in range(depth):
                            cur = words[i]
                            mixed = jnp.where(two, prev2, jnp.where(one, prev1, cur))
                            moved = jnp.take_along_axis(mixed, source, axis=1)
                            row = i * comps + c
                            acc[row] += weight * jnp.left_shift(moved, 16).astype(jnp.float32)
                            acc[row + half] += weight * moved.astype(jnp.float32)
                            prev2, prev1 = prev1, cur
            for q in range(rows):
                motion[comps + q, part, :] = acc[q]

    def sources(t):
        ring = t // chip
        k = (ring + 1) // 2
        q = z + jnp.where(ring % 2 == 1, -toward, toward) * k
        return q, q * plane + ((i_own // 2 + t) % chip) * 2

    def await_traces(first):
        @pl.when(first == me // 2 * 2)
        def _():
            mate = trace_bytes.at[pl.ds(0, cap * points * half + 1)]
            pltpu.make_async_copy(mate, mate, recv_t.at[first // 2]).wait()

        @pl.when(first != me // 2 * 2)
        def _():
            pltpu.make_async_copy(trace_bytes, trace_bytes, recv_t.at[first // 2]).wait()

    def arrive(t, carry):
        q, first = sources(t)

        @pl.when(inside(q))
        def _():
            await_traces(first)
            add_traces([first, first + 1], range(variations // 8))

        return carry

    def convolve(v):
        lhs = jnp.concatenate([motion[comps:comps + rows, v, :], motion[0:rows, v, :]], axis=1)
        high = lhs.astype(jnp.bfloat16).astype(jnp.float32)
        pair = jnp.concatenate([high, lhs - high], axis=0).astype(jnp.bfloat16)
        main = jnp.dot(pair, high_taps[v], preferred_element_type=jnp.float32)
        minor = jnp.dot(pair[:rows], low_taps[v], preferred_element_type=jnp.float32)
        out_ref[v] = main[:rows] + (main[rows:] + minor)

    lax.fori_loop(0, 6, encode_step, 0)
    encode_own()
    to_scalar.wait()
    early = jnp.where(inside(z + toward * (planes - 1)), chip if planes > 1 else 0, 0)
    lax.fori_loop(0, early, arrive, 0)
    lax.fori_loop(6, steps, encode_step, 0)
    last = 2 * jnp.where(toward > 0, planes - 1 - z, z) * chip + chip - 1
    lax.fori_loop(early, last, arrive, 0)
    _, first = sources(last)
    await_traces(first)
    for group in range(variations // 8):
        add_traces([first, first + 1], [group])
        for v in range(group * 8, group * 8 + 8):
            convolve(v)

    others = pl.ds(0, n - 1)
    for box, sem in ((want_v, send_m), (gain_v, send_m), (outbox, send_t), (out_scale, send_t)):
        pltpu.make_async_copy(box.at[others], box.at[others], sem).wait()


def local(plane, green_tensors, block_lists, block_count, onset_steps, slip_amount, mechanism, slip_rate):
    held, points, strains, comps, length = green_tensors.shape
    ruptures, listed = block_lists.shape
    assert ruptures == 1
    variations = onset_steps.shape[1]
    n = lax.axis_size("pts")
    cap = max(1, listed // n)
    tiles = length // LANES
    rows = tiles * comps
    assert n * cap <= LANES and listed * points <= LANES and rows == 16 and variations % 8 == 0
    green = green_tensors.reshape(held, points, strains, comps, tiles, LANES)
    green = green.transpose(0, 1, 2, 4, 3, 5).reshape(held, points, strains, rows, LANES)

    hbm = pl.BlockSpec(memory_space=pltpu.MemorySpace.HBM)
    vmem = pl.BlockSpec(memory_space=pltpu.VMEM)
    dma = pltpu.SemaphoreType.DMA
    planes = n // plane
    seismograms = pl.pallas_call(
        functools.partial(seismogram_kernel, n, plane, cap, held, points, comps),
        out_shape=jax.ShapeDtypeStruct((variations, rows, LANES), jnp.float32),
        in_specs=[pl.BlockSpec(memory_space=pltpu.SMEM)] + [hbm] * 6,
        out_specs=vmem,
        scratch_shapes=[
            pltpu.VMEM((1, listed), jnp.int32),
            pltpu.VMEM((1, strains), jnp.float32),
            pltpu.VMEM((1, LANES), jnp.float32),
            pltpu.VMEM((held, points, strains, rows, LANES), jnp.bfloat16),
            pltpu.VMEM((variations, listed * points), jnp.int32),
            pltpu.VMEM((variations, listed * points), jnp.float32),
            pltpu.VMEM((variations, LANES), jnp.float32),
            pltpu.VMEM((n, cap, LANES), jnp.int32),
            pltpu.VMEM((1, LANES), jnp.int32),
            pltpu.SMEM((1, LANES), jnp.int32),
            pltpu.VMEM((n, cap, LANES), jnp.int32),
            pltpu.VMEM((n, 1, LANES), jnp.float32),
            pltpu.VMEM((n, cap, points, rows // 2, LANES), jnp.int32),
            pltpu.VMEM((n, 1, LANES), jnp.float32),
            pltpu.VMEM((n, cap, points, rows // 2, LANES), jnp.int32),
            pltpu.VMEM((n, 1, LANES), jnp.float32),
            pltpu.VMEM((rows + comps, variations, LANES), jnp.float32),
            pltpu.VMEM((variations, 2 * LANES, LANES), jnp.bfloat16),
            pltpu.VMEM((variations, 2 * LANES, LANES), jnp.bfloat16),
            pltpu.VMEM(((listed + 1) * points, variations, LANES), jnp.int32),
            pltpu.VMEM(((listed + 1) * points, variations, LANES), jnp.int32),
            pltpu.VMEM(((listed + 1) * points, variations, LANES), jnp.float32),
            pltpu.VMEM((plane // 2 * (cap + 1), 1, LANES), jnp.int32),
            pltpu.VMEM((2 * (cap * points * rows // 2 + 1), 1, LANES), jnp.int32),
            dma((7,)), pltpu.SemaphoreType.REGULAR((planes,)), dma, dma((2 * planes,)), dma, dma((n // 2,)),
        ],
        compiler_params=pltpu.CompilerParams(
            collective_id=0, has_side_effects=True, vmem_limit_bytes=32 << 20),
        name="seismograms",
    )(block_count, *(pltpu.with_memory_space_constraint(x, pltpu.MemorySpace.HBM) for x in (
        block_lists, mechanism, green, onset_steps[0], slip_amount[0], slip_rate[0])))
    out = seismograms.reshape(variations, tiles, comps, LANES).transpose(0, 2, 1, 3)
    return out.reshape(1, variations, comps, length)


def solution(mesh):
    n = mesh.shape["pts"]
    line = mesh.devices.reshape(-1, n)[0]
    heights = [getattr(d, "coords", (0, 0, 0))[2] for d in line]
    plane = sum(1 for h in heights if h == heights[0])
    assert n % plane == 0 and plane % 2 == 0
    in_specs = (
        P(("site", "pts"), None, None, None, None),
        P(("site", "pts"), None),
        P(("site", "pts")),
        P(("site", "pts"), None, None),
        P(("site", "pts"), None, None),
        P(("site", "pts"), None),
        P(("site", "pts"), None, None),
    )
    out_specs = P(("site", "pts"), None, None, None)
    return jax.shard_map(functools.partial(local, plane), mesh=mesh, in_specs=in_specs, out_specs=out_specs,
                         check_vma=False)
```
